32 devices in a mesh: row: 16 (over z, y, x), col: 2 (over core).
Axes of the slice: x: 2, y: 2, z: 4, core: 2. Of those that a mesh axis runs over, the one named last changes fastest.
Arguments:
- block_ids: int32 [64, 8], replicated, may hold values from 0 to 383, as said below
- iface_counts: int32 [64], replicated, may hold values from 6 to 8
- inv_factor: bfloat16 [30208, 472], P(('row', 'col')), as said below
- coupling: bfloat16 [30208, 1024], P(('row', 'col')), may hold values from -0.375 to 0.375
- boundary_block: bfloat16 [24, 2048, 8, 256], P(None, 'row', None, 'col'), may hold values from -6 to 6
Outputs:
- schur: float32 [24, 2048, 8, 256], P(None, 'row', None, 'col')
The draws below stay inside these ranges and needn't reach their ends.
Inputs may be any that keep to these rules, and one draw needn't show every extreme that they name: For j < 2, block_ids[s, j] is below 16, equals (s // 2 + j) modulo 2, and is the same for the 2 substructures that share s // 2. Apart from these shared first 2 ids, the ids of the 2 substructures that share s // 2 are distinct modulo 16. `inv_factor`: each substructure's block is lower triangular with a diagonal from 0.5 to 1.5.
All inputs are finite; a program needn't handle non-finite values.
Results may differ from the reference program's by a relative error of at most 0.00044.
Values sent between devices are 32-bit elements; how exact they have to be, the bound alone decides.
A program may use at most 64 MiB of HBM per device.

```python
import jax
import jax.numpy as jnp
from jax import lax

NI = 472
NB = 8
CS = 2
NQ = 24
CB = 16
SD = 2
SUBS = 64
CQ = 8
N_ROW = 16
N_COL = 2


def draw_block_ids(key, part):
    places = N_ROW * N_COL
    member = jnp.arange(places, dtype=jnp.int32) % N_COL
    keys = jax.random.split(jax.random.fold_in(key, 11), 3)
    columns = jnp.stack([(member + j) % N_COL for j in range(CS)], axis=1)
    depth = jax.random.randint(keys[0], (places, CS), 0, CB // N_COL)
    span_ids = columns + N_COL * depth
    used = jnp.any((span_ids % N_ROW)[:, :, None] == jnp.arange(N_ROW, dtype=jnp.int32)[None, None, :], axis=1)
    scores = jax.random.randint(keys[1], (places, N_ROW), 0, 2 ** 20) * N_ROW + jnp.arange(N_ROW, dtype=jnp.int32)[None, :]
    scores = scores + used.astype(jnp.int32) * 2 ** 26
    order = jnp.argsort(scores, axis=1)
    owners = order[:, :SD * (NB - CS)].astype(jnp.int32).reshape(places, SD, NB - CS)
    others = owners + N_ROW * jax.random.randint(keys[2], (places, SD, NB - CS), 0, NQ)
    shared = jnp.broadcast_to(span_ids[:, None, :], (places, SD, CS))
    return jnp.concatenate([shared, others], axis=2).reshape(places * SD, NB).astype(jnp.int32)


def draw_inv_factor(key, part):
    subs = SD * N_ROW * N_COL
    first, second = jax.random.split(jax.random.fold_in(key, 23))
    spread = jax.random.normal(first, (subs, NI, NI), jnp.float32)
    lower = jnp.tril(jnp.ones((NI, NI), jnp.float32), -1)
    pivots = jax.random.uniform(second, (subs, NI), jnp.float32, 0.5, 1.5)
    matrix = spread * lower[None] * NI ** (-0.5) + pivots[:, :, None] * jnp.eye(NI, dtype=jnp.float32)[None]
    return matrix.reshape(subs * NI, NI).astype(jnp.bfloat16)


def plant(drawn, own_key, low, top_value):
    spot = [jax.random.randint(jax.random.fold_in(own_key, axis), (), 0, length) for axis, length in enumerate(drawn.shape)]
    widest = drawn.shape.index(max(drawn.shape))
    neighbour = spot[:widest] + [(spot[widest] + 1) % drawn.shape[widest]] + spot[widest + 1:]
    return drawn.at[tuple(spot)].set(low).at[tuple(neighbour)].set(top_value)


def shard_levels(rng, extent, pieces, least, high):
    factor_of = 1.0
    for position, shards_of in pieces:
        steps = jax.random.uniform(jax.random.fold_in(jax.random.fold_in(rng, 6), position), (shards_of,), jnp.float32, least / len(pieces), high / len(pieces))
        factor_of = factor_of * jnp.repeat(jnp.exp(steps), extent[position] // shards_of).reshape((-1,) + (1,) * (len(extent) - 1 - position))
    return factor_of


def noise(own_key, extent, scale, bound, pieces=(), kind=jnp.bfloat16):
    result = jax.random.normal(own_key, extent, jnp.float32) * scale
    if len(pieces) > 0:
        result = shard_levels(own_key, extent, pieces, -0.22, 0.18) * result
    return jnp.clip(result, min=-bound, max=bound).astype(kind)


def setup_inputs(seed: int = 0) -> dict:
    key_list = jax.random.split(jax.random.key(seed), 6)
    block_ids = draw_block_ids(jax.random.fold_in(key_list[5], 71), 0)
    iface_counts = plant(jax.random.randint(key_list[1], (SUBS,), max(CS, NB - 2), NB + 1), jax.random.fold_in(key_list[1], 1), max(CS, NB - 2), NB).astype(jnp.int32)
    inv_factor = draw_inv_factor(jax.random.fold_in(key_list[5], 71), 0)
    coupling = noise(key_list[3], (SUBS * NI, NB * 128), (NI // 2) ** -0.5, 0.375, ((0, 32),))
    boundary_block = noise(key_list[4], (NQ, N_ROW * 128, CQ, N_COL * 128), 1.0, 6.0, ((1, 16), (3, 2)))
    return {"block_ids": block_ids, "iface_counts": iface_counts, "inv_factor": inv_factor, "coupling": coupling, "boundary_block": boundary_block}


def reference(block_ids, iface_counts, inv_factor, coupling, boundary_block):
    subs = SD * N_ROW * N_COL
    factors = inv_factor.reshape(subs, NI, NI)
    couples = coupling.reshape(subs, NI, NB * 128)
    total = jnp.zeros((NQ * N_ROW, 128, CB, 128), jnp.float32)

    def visit(total, item):
        factor, couple, ids, count = item
        mixed = jnp.dot(factor, couple, preferred_element_type=jnp.float32).astype(jnp.bfloat16)
        partial_value = lax.dot_general(mixed, mixed[:, :CS * 128], (((0,), (0,)), ((), ())), preferred_element_type=jnp.float32)
        live = (jnp.arange(NB, dtype=jnp.int32) < count).astype(jnp.float32)
        tiles = partial_value.reshape(NB, 128, CS, 128) * live[:, None, None, None]
        tiles = tiles.transpose(0, 2, 1, 3)
        total = total.at[ids[:, None], :, ids[None, :CS], :].add(tiles)
        return total, None

    total, unused = lax.scan(visit, total, (factors, couples, block_ids, iface_counts))
    dense = total.reshape(NQ * N_ROW * 128, CB * 128)
    given = boundary_block.astype(jnp.float32).reshape(NQ * N_ROW * 128, CB * 128)
    return (given - dense).reshape(NQ, N_ROW * 128, CB // N_COL, N_COL * 128)
```

```python
import functools

import jax
import jax.numpy as jnp
from jax import lax
from jax.experimental import pallas as pl
from jax.experimental.pallas import tpu as pltpu
from jax.sharding import PartitionSpec as P

CS = 2
MESH = pl.DeviceIdType.MESH


def exchange_kernel(
    rows, cols, members, slots, width, nq, cq,
    pieces,
    ids_ref, counts_ref, factor_ref, couple_ref, boundary_ref,
    head_ref, rest_ref, recv_ref, cells_ref,
    w_ref, k_ref, y_ref, p_ref, send_ref, given_ref, place_ref, cell_ref,
    load_sem, send_sem, recv_sem, given_sem, cell_sem,
):
    row_at = lax.axis_index("row")
    col_at = lax.axis_index("col")
    half = rows // 2
    side = row_at // half

    loads = []
    for m in range(members):
        loads.append(
            (
                pltpu.make_async_copy(factor_ref.at[m], w_ref.at[m], load_sem.at[2 * m]),
                pltpu.make_async_copy(couple_ref.at[m], k_ref.at[m], load_sem.at[2 * m + 1]),
            )
        )
        for load in loads[-1]:
            load.start()

    barrier = pltpu.get_barrier_semaphore()
    for r in range(1, rows):
        other = lax.rem(row_at + r, rows)
        pl.semaphore_signal(barrier, inc=1, device_id=(other, col_at), device_id_type=MESH)
    for r in range(rows):
        for j in range(1, CS):
            pl.semaphore_signal(
                barrier, inc=1, device_id=(r, lax.rem(col_at + j, cols)), device_id_type=MESH
            )
            if cols > 2:
                pl.semaphore_signal(
                    barrier, inc=1, device_id=(r, lax.rem(col_at + cols - j, cols)),
                    device_id_type=MESH,
                )

    given = pltpu.make_async_copy(boundary_ref, given_ref, given_sem)
    given.start()

    own = (row_at * cols + col_at) * members
    for m in range(members):
        for load in loads[m]:
            load.wait()
        for n in range(0, slots * 128, 256):
            y_ref[m, :, n : n + 256] = jnp.dot(
                w_ref[m], k_ref[m, :, n : n + 256], preferred_element_type=jnp.float32
            ).astype(jnp.bfloat16)
        for n in range(0, slots, 2):
            part = lax.dot_general(
                y_ref[m, :, n * 128 : n * 128 + 256],
                y_ref[m, :, 0 : CS * 128],
                (((0,), (0,)), ((), ())),
                preferred_element_type=jnp.float32,
            )
            for d in range(2):
                for j in range(CS):
                    p_ref[m * slots + n + d, j] = part[
                        d * 128 : (d + 1) * 128, j * 128 : (j + 1) * 128
                    ]

    fourth = rows // 4
    plane = row_at // fourth

    def within(at, i):
        return at * fourth + lax.rem(row_at + i, fourth)

    ends = [within(3 * (1 - side), i) for i in range(fourth)]
    middles = [within(2 - side, i) for i in range(fourth)]
    mates = [within(side * 2 + 1 - lax.rem(plane, 2), i) for i in range(fourth)]
    near = [within(plane, i) for i in range(1, fourth)]
    targets = [t for pair in zip(ends, mates) for t in pair]
    whole = len(targets)
    targets += [t for pair in zip(middles, near) for t in pair] + [middles[-1], row_at]

    partners = (rows - 1) + (CS - 1) * rows * (2 if cols > 2 else 1)
    def route(i, target, j, piece):
        start, height = pieces[piece]
        src = send_ref.at[pl.ds((j * rows + i) * 128 + start, height)]
        dst = recv_ref.at[pl.ds((j * rows + row_at) * 128 + start, height)]
        if j == 0 and i == rows - 1:
            return pltpu.make_async_copy(src, dst, recv_sem.at[piece])
        return pltpu.make_async_remote_copy(
            src_ref=src,
            dst_ref=dst,
            send_sem=send_sem,
            recv_sem=recv_sem.at[piece],
            device_id=(target, lax.rem(col_at + j, cols)),
            device_id_type=MESH,
        )

    for i, target in enumerate(targets):
        picks = []
        for m in range(members):
            k, weight = jnp.int32(0), jnp.float32(0.0)
            count = counts_ref[own + m]
            for kk in range(slots):
                hit = (lax.rem(ids_ref[kk, own + m], rows) == target) & (kk < count)
                k = jnp.where(hit, jnp.int32(kk), k)
                weight = jnp.where(hit, jnp.float32(1.0), weight)
            picks.append((m * slots + k, weight))
        for j in range(CS):
            total = p_ref[picks[0][0], j] * picks[0][1]
            for k, weight in picks[1:]:
                total = total + p_ref[k, j] * weight
            send_ref[(j * rows + i) * 128 : (j * rows + i + 1) * 128] = total
        if i == 1:
            pl.semaphore_wait(barrier, partners)
        if i >= 1:
            for j in range(CS):
                for piece in range(len(pieces) if i - 1 < whole else 1):
                    route(i - 1, targets[i - 1], j, piece).start()
    for j in range(CS):
        route(rows - 1, targets[-1], j, 0).start()
    for piece in range(1, len(pieces)):
        for i in range(whole, rows):
            for j in range(CS):
                route(i, targets[i], j, piece).start()

    wide = place_ref.shape[1]
    sources = CS * rows
    cell_iota = lax.broadcasted_iota(jnp.int32, (nq * cq, wide), 0)
    lane_iota = lax.broadcasted_iota(jnp.int32, (nq * cq, wide), 1)

    def add_source(r, cells):
        for j in range(CS):
            first = (r * cols + lax.rem(col_at + cols - j, cols)) * members
            cell = jnp.int32(-1)
            column = lax.div(ids_ref[j, first], cols)
            for m in range(members):
                for kk in range(slots):
                    if m > 0 and kk < CS:
                        continue
                    ident = ids_ref[kk, first + m]
                    cell = jnp.where(
                        lax.rem(ident, rows) == row_at,
                        lax.div(ident, rows) * cq + column,
                        cell,
                    )
            cell_ref[j * rows + r] = jnp.maximum(cell, 0)
            lane = lane_iota - (j * rows + r)
            cells = jnp.where((lane == 0) | (lane == sources), cell, cells)
        return cells

    cells = lax.fori_loop(0, rows, add_source, jnp.full((nq * cq, wide), -1, jnp.int32))
    place_ref[...] = (cells == cell_iota).astype(jnp.float32).astype(jnp.bfloat16)

    listed = pltpu.make_async_copy(cell_ref, cells_ref, cell_sem)
    listed.start()

    given.wait()
    start, height = pieces[1]

    def widen(q, carry):
        rest_ref[q] = given_ref[q, start:].astype(jnp.float32).reshape(height * cq, 128)
        return carry

    lax.fori_loop(0, nq, widen, 0)
    listed.wait()

    def arrive(piece):
        arrived = recv_ref.at[pl.ds(0, sources * pieces[piece][1])]
        pltpu.make_async_copy(arrived, arrived, recv_sem.at[piece]).wait()

    arrive(0)
    place = place_ref[...]

    def place_rows(step, carry):
        first = step * 4
        halves = []
        for a in range(4):
            line = recv_ref[pl.ds(first + a, sources, stride=128), :]
            high = line.astype(jnp.bfloat16)
            low = (line - high.astype(jnp.float32)).astype(jnp.bfloat16)
            halves.append(jnp.concatenate([high, low], axis=0))
        for a in range(0, 4, 2):
            both = jnp.concatenate(halves[a : a + 2], axis=1)
            total = jnp.dot(place, both, preferred_element_type=jnp.float32)
            for d in range(2):
                head_ref[:, pl.ds((first + a + d) * cq, cq)] = given_ref[:, first + a + d].astype(
                    jnp.float32
                ) - total[:, d * 128 : (d + 1) * 128].reshape(nq, cq, 128)
        return carry

    lax.fori_loop(0, pieces[0][1] // 4, place_rows, 0)
    arrive(1)
    sent = send_ref.at[pl.ds(0, (sources - 1) * 128)]
    pltpu.make_async_copy(sent, sent, send_sem).wait()


def write_kernel(
    sources, cq, pieces,
    head_ref, given_ref, recv_ref, cells_ref,
    out_ref, rest_ref,
    cell_ref, cell_sem, sem,
):
    listed = pltpu.make_async_copy(cells_ref, cell_ref, cell_sem)
    listed.start()
    nq = head_ref.shape[0]
    split = 2
    for i in range(split):
        part = pl.ds(i * (nq // split), nq // split)
        pltpu.make_async_copy(
            head_ref.at[part], out_ref.at[part, pl.ds(0, pieces[0][1] * cq)], sem
        ).start()
    listed.wait()
    start, height = pieces[1]

    def settle(s, carry):
        cell = cell_ref[s]
        q = lax.div(cell, cq)
        at = (q, pl.ds(lax.rem(cell, cq), height, stride=cq), slice(None))
        rest_ref[at] = rest_ref[at] - recv_ref[pl.ds(pl.multiple_of(s * 128, 128) + start, height)]
        return carry

    lax.fori_loop(0, sources, settle, 0)
    split = 4
    for i in range(split):
        part = pl.ds(i * (nq // split), nq // split)
        pltpu.make_async_copy(
            rest_ref.at[part], out_ref.at[part, pl.ds(start * cq, height * cq)], sem
        ).start()
    pltpu.make_async_copy(out_ref, out_ref, sem).wait()


def kept(value):
    return pltpu.with_memory_space_constraint(value, pltpu.HBM)


def on_device(rows, cols, block_ids, iface_counts, inv_factor, coupling, boundary_block):
    slots = block_ids.shape[1]
    width = inv_factor.shape[1]
    members = inv_factor.shape[0] // width
    nq, tall, cq, _ = boundary_block.shape
    sources = CS * rows
    pieces = ((0, 32), (32, 96))
    head, rest, landed, cells = pl.pallas_call(
        functools.partial(exchange_kernel, rows, cols, members, slots, width, nq, cq, pieces),
        out_shape=(
            jax.ShapeDtypeStruct((nq, pieces[0][1] * cq, 128), jnp.float32),
            jax.ShapeDtypeStruct((nq, pieces[1][1] * cq, 128), jnp.float32),
            jax.ShapeDtypeStruct((sources * 128, 128), jnp.float32),
            jax.ShapeDtypeStruct((sources,), jnp.int32),
        ),
        in_specs=[
            pl.BlockSpec(memory_space=pltpu.SMEM),
            pl.BlockSpec(memory_space=pltpu.SMEM),
            pl.BlockSpec(memory_space=pltpu.HBM),
            pl.BlockSpec(memory_space=pltpu.HBM),
            pl.BlockSpec(memory_space=pltpu.HBM),
        ],
        out_specs=(
            pl.BlockSpec(memory_space=pltpu.VMEM),
            pl.BlockSpec(memory_space=pltpu.VMEM),
            pl.BlockSpec(memory_space=pltpu.VMEM),
            pl.BlockSpec(memory_space=pltpu.HBM),
        ),
        scratch_shapes=[
            pltpu.VMEM((members, width, width), jnp.bfloat16),
            pltpu.VMEM((members, width, slots * 128), jnp.bfloat16),
            pltpu.VMEM((members, width, slots * 128), jnp.bfloat16),
            pltpu.VMEM((members * slots, CS, 128, 128), jnp.float32),
            pltpu.VMEM((sources * 128, 128), jnp.float32),
            pltpu.VMEM(boundary_block.shape, jnp.bfloat16),
            pltpu.VMEM((nq * cq, 2 * sources), jnp.bfloat16),
            pltpu.SMEM((sources,), jnp.int32),
            pltpu.SemaphoreType.DMA((2 * members,)),
            pltpu.SemaphoreType.DMA,
            pltpu.SemaphoreType.DMA((len(pieces),)),
            pltpu.SemaphoreType.DMA,
            pltpu.SemaphoreType.DMA,
        ],
        compiler_params=pltpu.CompilerParams(
            collective_id=0, has_side_effects=True, vmem_limit_bytes=32 * 1024 * 1024
        ),
        name="exchange",
    )(
        kept(block_ids.T),
        kept(iface_counts),
        kept(inv_factor.reshape(members, width, width)),
        kept(coupling.reshape(members, width, slots * 128)),
        kept(boundary_block),
    )
    result, _ = pl.pallas_call(
        functools.partial(write_kernel, sources, cq, pieces),
        out_shape=(
            jax.ShapeDtypeStruct((nq, tall * cq, 128), jnp.float32),
            jax.ShapeDtypeStruct(rest.shape, jnp.float32),
        ),
        in_specs=[
            pl.BlockSpec(memory_space=pltpu.VMEM),
            pl.BlockSpec(memory_space=pltpu.VMEM),
            pl.BlockSpec(memory_space=pltpu.VMEM),
            pl.BlockSpec(memory_space=pltpu.HBM),
        ],
        out_specs=(
            pl.BlockSpec(memory_space=pltpu.HBM),
            pl.BlockSpec(memory_space=pltpu.VMEM),
        ),
        input_output_aliases={1: 1},
        scratch_shapes=[
            pltpu.SMEM((sources,), jnp.int32),
            pltpu.SemaphoreType.DMA,
            pltpu.SemaphoreType.DMA,
        ],
        compiler_params=pltpu.CompilerParams(vmem_limit_bytes=16 * 1024 * 1024),
        name="writing",
    )(head, rest, landed, cells)
    return result.reshape(boundary_block.shape)


def solution(mesh):
    return jax.shard_map(
        functools.partial(on_device, mesh.shape["row"], mesh.shape["col"]),
        mesh=mesh,
        in_specs=(
            P(),
            P(),
            P(("row", "col"), None),
            P(("row", "col"), None),
            P(None, "row", None, "col"),
        ),
        out_specs=P(None, "row", None, "col"),
        check_vma=False,
    )
```

```python
import functools

import jax
import jax.numpy as jnp
from jax import lax
from jax.experimental import pallas as pl
from jax.experimental.pallas import tpu as pltpu
from jax.sharding import PartitionSpec as P

CS = 2
MESH = pl.DeviceIdType.MESH


def exchange_kernel(
    rows, cols, members, slots, width, nq, cq,
    pieces,
    ids_ref, counts_ref, factor_ref, couple_ref, boundary_ref,
    head_ref, rest_ref, recv_ref, cells_ref,
    w_ref, k_ref, y_ref, p_ref, send_ref, given_ref, place_ref, cell_ref,
    load_sem, send_sem, recv_sem, given_sem, cell_sem, ready_sem,
):
    row_at = lax.axis_index("row")
    col_at = lax.axis_index("col")
    half = rows // 2
    side = row_at // half

    loads = []
    for m in range(members):
        loads.append([pltpu.make_async_copy(factor_ref.at[m], w_ref.at[m], load_sem.at[m, slots])])
        for k in range(slots):
            loads[m].append(
                pltpu.make_async_copy(
                    couple_ref.at[m, :, pl.ds(k * 128, 128)],
                    k_ref.at[m * slots + k],
                    load_sem.at[m, k],
                )
            )
        for load in loads[m]:
            load.start()

    fourth = rows // 4
    plane = row_at // fourth
    sides = (0, 1) if cols == 2 else (0, 1, cols - 1)

    def within(at, i):
        return at * fourth + lax.rem(row_at + i, fourth)

    barrier = pltpu.get_barrier_semaphore()
    for hop in range(4):
        for j in sides:
            if hop or j:
                pl.semaphore_signal(
                    barrier, inc=1,
                    device_id=(
                        lax.rem(row_at + hop * fourth, rows), lax.rem(col_at + j, cols)
                    ),
                    device_id_type=MESH,
                )
    for i in range(1, fourth):
        pl.semaphore_signal(
            barrier, inc=1, device_id=(within(plane, i), col_at), device_id_type=MESH
        )

    def columns(m, k):
        return jnp.concatenate([k_ref[m * slots + k], k_ref[m * slots + k + 1]], axis=1)

    own = (row_at * cols + col_at) * members
    for m in range(members):
        for load in loads[m]:
            load.wait()
        y_ref[m, :, 0 : CS * 128] = jnp.dot(
            w_ref[m], columns(m, 0), preferred_element_type=jnp.float32
        ).astype(jnp.bfloat16)
    given = pltpu.make_async_copy(boundary_ref, given_ref, given_sem)
    given.start()

    ends = [within(3 * (1 - side), i) for i in range(fourth)]
    middles = [within(2 - side, i) for i in range(fourth)]
    mates = [within(side * 2 + 1 - lax.rem(plane, 2), i) for i in range(fourth)]
    near = [within(plane, i) for i in range(1, fourth)]
    targets = [ends[0], middles[0]]
    early = len(targets)
    targets += [t for pair in zip(mates, ends[1:]) for t in pair] + [mates[-1]]
    whole = len(targets)
    targets += [t for pair in zip(near, middles[1:]) for t in pair] + [row_at]

    def route(i, target, j, piece):
        start, height = pieces[piece]
        src = send_ref.at[pl.ds((j * rows + i) * 128 + start, height)]
        dst = recv_ref.at[pl.ds((j * rows + row_at) * 128 + start, height)]
        if j == 0 and i == rows - 1:
            return pltpu.make_async_copy(src, dst, recv_sem.at[piece])
        return pltpu.make_async_remote_copy(
            src_ref=src,
            dst_ref=dst,
            send_sem=send_sem,
            recv_sem=recv_sem.at[piece],
            device_id=(target, lax.rem(col_at + j, cols)),
            device_id_type=MESH,
        )

    def launch(i):
        for j in range(CS):
            for piece in range(len(pieces) if i < whole else 1):
                route(i, targets[i], j, piece).start()

    def pick(target):
        picks = []
        for m in range(members):
            k, weight = jnp.int32(0), jnp.float32(0.0)
            count = counts_ref[own + m]
            for kk in range(slots):
                hit = (lax.rem(ids_ref[kk, own + m], rows) == target) & (kk < count)
                k = jnp.where(hit, jnp.int32(kk), k)
                weight = jnp.where(hit, jnp.float32(1.0), weight)
            picks.append((k, weight))
        return picks

    for i in range(early):
        total = None
        for m, (k, weight) in enumerate(pick(targets[i])):
            block = jnp.dot(
                w_ref[m],
                k_ref[m * slots + k],
                preferred_element_type=jnp.float32,
            ).astype(jnp.bfloat16)
            part = lax.dot_general(
                block,
                y_ref[m, :, 0 : CS * 128],
                (((0,), (0,)), ((), ())),
                preferred_element_type=jnp.float32,
            ) * weight
            total = part if total is None else total + part
        for j in range(CS):
            send_ref[(j * rows + i) * 128 : (j * rows + i + 1) * 128] = total[
                :, j * 128 : (j + 1) * 128
            ]
        if i == 0:
            pl.semaphore_wait(barrier, 4 * len(sides) - 1 + fourth - 1)
            for n in range(1, fourth):
                pl.semaphore_signal(
                    ready_sem, inc=1, device_id=(within(plane, n), col_at), device_id_type=MESH
                )
        launch(i)

    for m in range(members):
        for n in range(CS * 128, slots * 128, 256):
            y_ref[m, :, n : n + 256] = jnp.dot(
                w_ref[m], columns(m, n // 128), preferred_element_type=jnp.float32
            ).astype(jnp.bfloat16)
        for n in range(0, slots, 2):
            part = lax.dot_general(
                y_ref[m, :, n * 128 : n * 128 + 256],
                y_ref[m, :, 0 : CS * 128],
                (((0,), (0,)), ((), ())),
                preferred_element_type=jnp.float32,
            )
            for d in range(2):
                for j in range(CS):
                    p_ref[m * slots + n + d, j] = part[
                        d * 128 : (d + 1) * 128, j * 128 : (j + 1) * 128
                    ]

    for i in range(early, rows):
        target = targets[i]
        picks = pick(target)
        for j in range(CS):
            total = p_ref[picks[0][0] + 0, j] * picks[0][1]
            for m in range(1, members):
                total = total + p_ref[m * slots + picks[m][0], j] * picks[m][1]
            send_ref[(j * rows + i) * 128 : (j * rows + i + 1) * 128] = total
        if i == early:
            pl.semaphore_wait(ready_sem, fourth - 1)
        else:
            launch(i - 1)
    launch(rows - 1)
    for piece in range(1, len(pieces)):
        for i in range(whole, rows):
            for j in range(CS):
                route(i, targets[i], j, piece).start()

    wide = place_ref.shape[1]
    sources = CS * rows
    cell_iota = lax.broadcasted_iota(jnp.int32, (nq * cq, wide), 0)
    lane_iota = lax.broadcasted_iota(jnp.int32, (nq * cq, wide), 1)

    def add_source(r, cells):
        for j in range(CS):
            first = (r * cols + lax.rem(col_at + cols - j, cols)) * members
            cell = jnp.int32(-1)
            column = lax.div(ids_ref[j, first], cols)
            for m in range(members):
                for kk in range(slots):
                    if m > 0 and kk < CS:
                        continue
                    ident = ids_ref[kk, first + m]
                    cell = jnp.where(
                        lax.rem(ident, rows) == row_at,
                        lax.div(ident, rows) * cq + column,
                        cell,
                    )
            cell_ref[j * rows + r] = jnp.maximum(cell, 0)
            lane = lane_iota - (j * rows + r)
            cells = jnp.where((lane == 0) | (lane == sources), cell, cells)
        return cells

    cells = lax.fori_loop(0, rows, add_source, jnp.full((nq * cq, wide), -1, jnp.int32))
    place_ref[...] = (cells == cell_iota).astype(jnp.float32).astype(jnp.bfloat16)

    listed = pltpu.make_async_copy(cell_ref, cells_ref, cell_sem)
    listed.start()

    given.wait()
    start, height = pieces[1]

    def widen(q, carry):
        rest_ref[q] = given_ref[q, start:].astype(jnp.float32).reshape(height * cq, 128)
        return carry

    lax.fori_loop(0, nq, widen, 0)
    listed.wait()

    def arrive(piece):
        arrived = recv_ref.at[pl.ds(0, sources * pieces[piece][1])]
        pltpu.make_async_copy(arrived, arrived, recv_sem.at[piece]).wait()

    arrive(0)
    place = place_ref[...]

    def place_rows(step, carry):
        first = step * 4
        halves = []
        for a in range(4):
            line = recv_ref[pl.ds(first + a, sources, stride=128), :]
            high = line.astype(jnp.bfloat16)
            low = (line - high.astype(jnp.float32)).astype(jnp.bfloat16)
            halves.append(jnp.concatenate([high, low], axis=0))
        for a in range(0, 4, 2):
            both = jnp.concatenate(halves[a : a + 2], axis=1)
            total = jnp.dot(place, both, preferred_element_type=jnp.float32)
            for d in range(2):
                head_ref[:, pl.ds((first + a + d) * cq, cq)] = given_ref[:, first + a + d].astype(
                    jnp.float32
                ) - total[:, d * 128 : (d + 1) * 128].reshape(nq, cq, 128)
        return carry

    lax.fori_loop(0, pieces[0][1] // 4, place_rows, 0)
    arrive(1)
    sent = send_ref.at[pl.ds(0, (sources - 1) * 128)]
    pltpu.make_async_copy(sent, sent, send_sem).wait()


def write_kernel(
    sources, cq, pieces,
    head_ref, given_ref, recv_ref, cells_ref,
    out_ref, rest_ref,
    cell_ref, cell_sem, sem,
):
    listed = pltpu.make_async_copy(cells_ref, cell_ref, cell_sem)
    listed.start()
    nq = head_ref.shape[0]
    split = 2
    for i in range(split):
        part = pl.ds(i * (nq // split), nq // split)
        pltpu.make_async_copy(
            head_ref.at[part], out_ref.at[part, pl.ds(0, pieces[0][1] * cq)], sem
        ).start()
    listed.wait()
    start, height = pieces[1]

    def settle(s, carry):
        cell = cell_ref[s]
        q = lax.div(cell, cq)
        at = (q, pl.ds(lax.rem(cell, cq), height, stride=cq), slice(None))
        rest_ref[at] = rest_ref[at] - recv_ref[pl.ds(pl.multiple_of(s * 128, 128) + start, height)]
        return carry

    lax.fori_loop(0, sources, settle, 0)
    split = 4
    for i in range(split):
        part = pl.ds(i * (nq // split), nq // split)
        pltpu.make_async_copy(
            rest_ref.at[part], out_ref.at[part, pl.ds(start * cq, height * cq)], sem
        ).start()
    pltpu.make_async_copy(out_ref, out_ref, sem).wait()


def kept(value):
    return pltpu.with_memory_space_constraint(value, pltpu.HBM)


def on_device(rows, cols, block_ids, iface_counts, inv_factor, coupling, boundary_block):
    slots = block_ids.shape[1]
    width = inv_factor.shape[1]
    members = inv_factor.shape[0] // width
    nq, tall, cq, _ = boundary_block.shape
    sources = CS * rows
    pieces = ((0, 48), (48, 80))
    head, rest, landed, cells = pl.pallas_call(
        functools.partial(exchange_kernel, rows, cols, members, slots, width, nq, cq, pieces),
        out_shape=(
            jax.ShapeDtypeStruct((nq, pieces[0][1] * cq, 128), jnp.float32),
            jax.ShapeDtypeStruct((nq, pieces[1][1] * cq, 128), jnp.float32),
            jax.ShapeDtypeStruct((sources * 128, 128), jnp.float32),
            jax.ShapeDtypeStruct((sources,), jnp.int32),
        ),
        in_specs=[
            pl.BlockSpec(memory_space=pltpu.SMEM),
            pl.BlockSpec(memory_space=pltpu.SMEM),
            pl.BlockSpec(memory_space=pltpu.HBM),
            pl.BlockSpec(memory_space=pltpu.HBM),
            pl.BlockSpec(memory_space=pltpu.HBM),
        ],
        out_specs=(
            pl.BlockSpec(memory_space=pltpu.VMEM),
            pl.BlockSpec(memory_space=pltpu.VMEM),
            pl.BlockSpec(memory_space=pltpu.VMEM),
            pl.BlockSpec(memory_space=pltpu.HBM),
        ),
        scratch_shapes=[
            pltpu.VMEM((members, width, width), jnp.bfloat16),
            pltpu.VMEM((members * slots, width, 128), jnp.bfloat16),
            pltpu.VMEM((members, width, slots * 128), jnp.bfloat16),
            pltpu.VMEM((members * slots, CS, 128, 128), jnp.float32),
            pltpu.VMEM((sources * 128, 128), jnp.float32),
            pltpu.VMEM(boundary_block.shape, jnp.bfloat16),
            pltpu.VMEM((nq * cq, 2 * sources), jnp.bfloat16),
            pltpu.SMEM((sources,), jnp.int32),
            pltpu.SemaphoreType.DMA((members, slots + 1)),
            pltpu.SemaphoreType.DMA,
            pltpu.SemaphoreType.DMA((len(pieces),)),
            pltpu.SemaphoreType.DMA,
            pltpu.SemaphoreType.DMA,
            pltpu.SemaphoreType.REGULAR,
        ],
        compiler_params=pltpu.CompilerParams(
            collective_id=0, has_side_effects=True, vmem_limit_bytes=32 * 1024 * 1024
        ),
        name="exchange",
    )(
        kept(block_ids.T),
        kept(iface_counts),
        kept(inv_factor.reshape(members, width, width)),
        kept(coupling.reshape(members, width, slots * 128)),
        kept(boundary_block),
    )
    result, _ = pl.pallas_call(
        functools.partial(write_kernel, sources, cq, pieces),
        out_shape=(
            jax.ShapeDtypeStruct((nq, tall * cq, 128), jnp.float32),
            jax.ShapeDtypeStruct(rest.shape, jnp.float32),
        ),
        in_specs=[
            pl.BlockSpec(memory_space=pltpu.VMEM),
            pl.BlockSpec(memory_space=pltpu.VMEM),
            pl.BlockSpec(memory_space=pltpu.VMEM),
            pl.BlockSpec(memory_space=pltpu.HBM),
        ],
        out_specs=(
            pl.BlockSpec(memory_space=pltpu.HBM),
            pl.BlockSpec(memory_space=pltpu.VMEM),
        ),
        input_output_aliases={1: 1},
        scratch_shapes=[
            pltpu.SMEM((sources,), jnp.int32),
            pltpu.SemaphoreType.DMA,
            pltpu.SemaphoreType.DMA,
        ],
        compiler_params=pltpu.CompilerParams(vmem_limit_bytes=16 * 1024 * 1024),
        name="writing",
    )(head, rest, landed, cells)
    return result.reshape(boundary_block.shape)


def solution(mesh):
    return jax.shard_map(
        functools.partial(on_device, mesh.shape["row"], mesh.shape["col"]),
        mesh=mesh,
        in_specs=(
            P(),
            P(),
            P(("row", "col"), None),
            P(("row", "col"), None),
            P(None, "row", None, "col"),
        ),
        out_specs=P(None, "row", None, "col"),
        check_vma=False,
    )
```

```python
import functools

import jax
import jax.numpy as jnp
from jax import lax
from jax.experimental import pallas as pl
from jax.experimental.pallas import tpu as pltpu
from jax.sharding import PartitionSpec as P

CS = 2
MESH = pl.DeviceIdType.MESH


def exchange_kernel(
    rows, cols, members, slots, width, nq, cq,
    pieces,
    listed_ids_ref, listed_counts_ref, factor_ref, couple_ref, boundary_ref,
    head_ref, rest_ref, recv_ref, cells_ref,
    ids_ref, counts_ref, w_ref, k_ref, y_ref, p_ref, send_ref, given_ref, place_ref, cell_ref,
    list_sem, load_sem, send_sem, recv_sem, given_sem, cell_sem, ready_sem,
):
    row_at = lax.axis_index("row")
    col_at = lax.axis_index("col")
    half = rows // 2
    side = row_at // half

    lists = (
        pltpu.make_async_copy(listed_ids_ref, ids_ref, list_sem.at[0]),
        pltpu.make_async_copy(listed_counts_ref, counts_ref, list_sem.at[1]),
    )
    for load in lists:
        load.start()
    loads = []
    for m in range(members):
        loads.append([pltpu.make_async_copy(factor_ref.at[m], w_ref.at[m], load_sem.at[m, slots])])
        for k in range(slots):
            loads[m].append(
                pltpu.make_async_copy(
                    couple_ref.at[m, :, pl.ds(k * 128, 128)],
                    k_ref[m].at[k],
                    load_sem.at[m, k],
                )
            )
        for load in loads[m]:
            load.start()

    fourth = rows // 4
    plane = row_at // fourth
    sides = (0, 1) if cols == 2 else (0, 1, cols - 1)

    def within(at, i):
        return at * fourth + lax.rem(row_at + i, fourth)

    barrier = pltpu.get_barrier_semaphore()
    for hop in range(4):
        for j in sides:
            if hop or j:
                pl.semaphore_signal(
                    barrier, inc=1,
                    device_id=(
                        lax.rem(row_at + hop * fourth, rows), lax.rem(col_at + j, cols)
                    ),
                    device_id_type=MESH,
                )
    for i in range(1, fourth):
        pl.semaphore_signal(
            barrier, inc=1, device_id=(within(plane, i), col_at), device_id_type=MESH
        )

    def columns(m, k):
        return jnp.concatenate([k_ref[m][k], k_ref[m][k + 1]], axis=1)

    own = (row_at * cols + col_at) * members
    ends = [within(3 * (1 - side), i) for i in range(fourth)]
    middles = [within(2 - side, i) for i in range(fourth)]
    mates = [within(side * 2 + 1 - lax.rem(plane, 2), i) for i in range(fourth)]
    near = [within(plane, i) for i in range(1, fourth)]
    targets = [ends[0], middles[0]]
    early = len(targets)
    targets += [t for pair in zip(mates, ends[1:]) for t in pair] + [mates[-1]]
    whole = len(targets)
    targets += [t for pair in zip(near, middles[1:]) for t in pair] + [row_at]

    def route(i, target, j, piece):
        start, height = pieces[piece]
        src = send_ref.at[pl.ds((j * rows + i) * 128 + start, height)]
        dst = recv_ref.at[pl.ds((j * rows + row_at) * 128 + start, height)]
        if j == 0 and i == rows - 1:
            return pltpu.make_async_copy(src, dst, recv_sem.at[piece])
        return pltpu.make_async_remote_copy(
            src_ref=src,
            dst_ref=dst,
            send_sem=send_sem,
            recv_sem=recv_sem.at[piece],
            device_id=(target, lax.rem(col_at + j, cols)),
            device_id_type=MESH,
        )

    def launch(i):
        for j in range(CS):
            for piece in range(len(pieces) if i < whole else 1):
                route(i, targets[i], j, piece).start()

    def pick(target):
        picks = []
        for m in range(members):
            k, weight = jnp.int32(0), jnp.float32(0.0)
            count = counts_ref[own + m]
            for kk in range(slots):
                hit = (lax.rem(ids_ref[kk, own + m], rows) == target) & (kk < count)
                k = jnp.where(hit, jnp.int32(kk), k)
                weight = jnp.where(hit, jnp.float32(1.0), weight)
            picks.append((k, weight))
        return picks

    for load in lists:
        load.wait()
    merged = 1
    picked = [pick(targets[i]) for i in range(early)]
    parts = []
    for m in range(members):
        for load in loads[m]:
            load.wait()
        blocks = [k_ref[m][k] for k in range(CS)]
        blocks += [k_ref[m][picked[i][m][0]] for i in range(merged)]
        made = jnp.dot(
            w_ref[m], jnp.concatenate(blocks, axis=1), preferred_element_type=jnp.float32
        ).astype(jnp.bfloat16)
        y_ref[m, :, 0 : CS * 128] = made[:, 0 : CS * 128]
        parts.append(
            lax.dot_general(
                made[:, CS * 128 :],
                made[:, 0 : CS * 128],
                (((0,), (0,)), ((), ())),
                preferred_element_type=jnp.float32,
            )
        )
    for i in range(early):
        if i >= merged:
            made = []
            for m in range(members):
                block = jnp.dot(
                    w_ref[m], k_ref[m][picked[i][m][0]], preferred_element_type=jnp.float32
                ).astype(jnp.bfloat16)
                made.append(
                    lax.dot_general(
                        block,
                        y_ref[m, :, 0 : CS * 128],
                        (((0,), (0,)), ((), ())),
                        preferred_element_type=jnp.float32,
                    )
                )
        else:
            made = [part[i * 128 : (i + 1) * 128] for part in parts]
        total = made[0] * picked[i][0][1]
        for m in range(1, members):
            total = total + made[m] * picked[i][m][1]
        for j in range(CS):
            send_ref[(j * rows + i) * 128 : (j * rows + i + 1) * 128] = total[
                :, j * 128 : (j + 1) * 128
            ]
        if i == 0:
            pl.semaphore_wait(barrier, 4 * len(sides) - 1 + fourth - 1)
            for n in range(1, fourth):
                pl.semaphore_signal(
                    ready_sem, inc=1, device_id=(within(plane, n), col_at), device_id_type=MESH
                )
        launch(i)
        if i == 0:
            given = pltpu.make_async_copy(boundary_ref, given_ref, given_sem)
            given.start()

    for m in range(members):
        for n in range(CS * 128, slots * 128, 256):
            y_ref[m, :, n : n + 256] = jnp.dot(
                w_ref[m], columns(m, n // 128), preferred_element_type=jnp.float32
            ).astype(jnp.bfloat16)
        for n in range(0, slots, 2):
            part = lax.dot_general(
                y_ref[m, :, n * 128 : n * 128 + 256],
                y_ref[m, :, 0 : CS * 128],
                (((0,), (0,)), ((), ())),
                preferred_element_type=jnp.float32,
            )
            for d in range(2):
                for j in range(CS):
                    p_ref[m * slots + n + d, j] = part[
                        d * 128 : (d + 1) * 128, j * 128 : (j + 1) * 128
                    ]

    for i in range(early, rows):
        target = targets[i]
        picks = pick(target)
        for j in range(CS):
            total = p_ref[picks[0][0] + 0, j] * picks[0][1]
            for m in range(1, members):
                total = total + p_ref[m * slots + picks[m][0], j] * picks[m][1]
            send_ref[(j * rows + i) * 128 : (j * rows + i + 1) * 128] = total
        if i == early:
            pl.semaphore_wait(ready_sem, fourth - 1)
        else:
            launch(i - 1)
    launch(rows - 1)
    for piece in range(1, len(pieces)):
        for i in range(whole, rows):
            for j in range(CS):
                route(i, targets[i], j, piece).start()

    wide = place_ref.shape[1]
    sources = CS * rows
    cell_iota = lax.broadcasted_iota(jnp.int32, (nq * cq, wide), 0)
    lane_iota = lax.broadcasted_iota(jnp.int32, (nq * cq, wide), 1)

    def add_source(r, cells):
        for j in range(CS):
            first = (r * cols + lax.rem(col_at + cols - j, cols)) * members
            cell = jnp.int32(-1)
            column = lax.div(ids_ref[j, first], cols)
            for m in range(members):
                for kk in range(slots):
                    if m > 0 and kk < CS:
                        continue
                    ident = ids_ref[kk, first + m]
                    cell = jnp.where(
                        lax.rem(ident, rows) == row_at,
                        lax.div(ident, rows) * cq + column,
                        cell,
                    )
            cell_ref[j * rows + r] = jnp.maximum(cell, 0)
            lane = lane_iota - (j * rows + r)
            cells = jnp.where((lane == 0) | (lane == sources), cell, cells)
        return cells

    cells = lax.fori_loop(0, rows, add_source, jnp.full((nq * cq, wide), -1, jnp.int32))
    place_ref[...] = (cells == cell_iota).astype(jnp.float32).astype(jnp.bfloat16)

    listed = pltpu.make_async_copy(cell_ref, cells_ref, cell_sem)
    listed.start()

    given.wait()
    start, height = pieces[1]

    def widen(q, carry):
        rest_ref[q] = given_ref[q, start:].astype(jnp.float32).reshape(height * cq, 128)
        return carry

    lax.fori_loop(0, nq, widen, 0)
    listed.wait()

    def arrive(piece):
        arrived = recv_ref.at[pl.ds(0, sources * pieces[piece][1])]
        pltpu.make_async_copy(arrived, arrived, recv_sem.at[piece]).wait()

    arrive(0)
    place = place_ref[...]

    def place_rows(step, carry):
        first = step * 4
        halves = []
        for a in range(4):
            line = recv_ref[pl.ds(first + a, sources, stride=128), :]
            high = line.astype(jnp.bfloat16)
            low = (line - high.astype(jnp.float32)).astype(jnp.bfloat16)
            halves.append(jnp.concatenate([high, low], axis=0))
        for a in range(0, 4, 2):
            both = jnp.concatenate(halves[a : a + 2], axis=1)
            total = jnp.dot(place, both, preferred_element_type=jnp.float32)
            for d in range(2):
                head_ref[:, pl.ds((first + a + d) * cq, cq)] = given_ref[:, first + a + d].astype(
                    jnp.float32
                ) - total[:, d * 128 : (d + 1) * 128].reshape(nq, cq, 128)
        return carry

    lax.fori_loop(0, pieces[0][1] // 4, place_rows, 0)
    arrive(1)
    sent = send_ref.at[pl.ds(0, (sources - 1) * 128)]
    pltpu.make_async_copy(sent, sent, send_sem).wait()


def write_kernel(
    sources, cq, pieces,
    head_ref, given_ref, recv_ref, cells_ref,
    out_ref, rest_ref,
    cell_ref, cell_sem, sem,
):
    listed = pltpu.make_async_copy(cells_ref, cell_ref, cell_sem)
    listed.start()
    nq = head_ref.shape[0]
    for q in range(nq):
        pltpu.make_async_copy(head_ref.at[q], out_ref.at[q, pl.ds(0, pieces[0][1] * cq)], sem).start()
    listed.wait()
    start, height = pieces[1]

    def settle(s, carry):
        cell = cell_ref[s]
        q = lax.div(cell, cq)
        at = (q, pl.ds(lax.rem(cell, cq), height, stride=cq), slice(None))
        rest_ref[at] = rest_ref[at] - recv_ref[pl.ds(pl.multiple_of(s * 128, 128) + start, height)]
        return carry

    lax.fori_loop(0, sources, settle, 0)
    for q in range(nq):
        pltpu.make_async_copy(
            rest_ref.at[q], out_ref.at[q, pl.ds(start * cq, height * cq)], sem
        ).start()
    pltpu.make_async_copy(out_ref, out_ref, sem).wait()


def kept(value):
    return pltpu.with_memory_space_constraint(value, pltpu.HBM)


def on_device(rows, cols, block_ids, iface_counts, inv_factor, coupling, boundary_block):
    slots = block_ids.shape[1]
    width = inv_factor.shape[1]
    members = inv_factor.shape[0] // width
    nq, tall, cq, _ = boundary_block.shape
    sources = CS * rows
    pieces = ((0, 48), (48, 80))
    head, rest, landed, cells = pl.pallas_call(
        functools.partial(exchange_kernel, rows, cols, members, slots, width, nq, cq, pieces),
        out_shape=(
            jax.ShapeDtypeStruct((nq, pieces[0][1] * cq, 128), jnp.float32),
            jax.ShapeDtypeStruct((nq, pieces[1][1] * cq, 128), jnp.float32),
            jax.ShapeDtypeStruct((sources * 128, 128), jnp.float32),
            jax.ShapeDtypeStruct((sources,), jnp.int32),
        ),
        in_specs=[
            pl.BlockSpec(memory_space=pltpu.HBM),
            pl.BlockSpec(memory_space=pltpu.HBM),
            pl.BlockSpec(memory_space=pltpu.HBM),
            pl.BlockSpec(memory_space=pltpu.HBM),
            pl.BlockSpec(memory_space=pltpu.HBM),
        ],
        out_specs=(
            pl.BlockSpec(memory_space=pltpu.VMEM),
            pl.BlockSpec(memory_space=pltpu.VMEM),
            pl.BlockSpec(memory_space=pltpu.VMEM),
            pl.BlockSpec(memory_space=pltpu.HBM),
        ),
        scratch_shapes=[
            pltpu.SMEM((slots, block_ids.shape[0]), jnp.int32),
            pltpu.SMEM((block_ids.shape[0],), jnp.int32),
            pltpu.VMEM((members, width, width), jnp.bfloat16),
            [pltpu.VMEM((slots, width, 128), jnp.bfloat16)] * members,
            pltpu.VMEM((members, width, slots * 128), jnp.bfloat16),
            pltpu.VMEM((members * slots, CS, 128, 128), jnp.float32),
            pltpu.VMEM((sources * 128, 128), jnp.float32),
            pltpu.VMEM(boundary_block.shape, jnp.bfloat16),
            pltpu.VMEM((nq * cq, 2 * sources), jnp.bfloat16),
            pltpu.SMEM((sources,), jnp.int32),
            pltpu.SemaphoreType.DMA((2,)),
            pltpu.SemaphoreType.DMA((members, slots + 1)),
            pltpu.SemaphoreType.DMA,
            pltpu.SemaphoreType.DMA((len(pieces),)),
            pltpu.SemaphoreType.DMA,
            pltpu.SemaphoreType.DMA,
            pltpu.SemaphoreType.REGULAR,
        ],
        compiler_params=pltpu.CompilerParams(
            collective_id=0, has_side_effects=True, vmem_limit_bytes=32 * 1024 * 1024
        ),
        name="exchange",
    )(
        kept(block_ids.T),
        kept(iface_counts),
        kept(inv_factor.reshape(members, width, width)),
        kept(coupling.reshape(members, width, slots * 128)),
        kept(boundary_block),
    )
    result, _ = pl.pallas_call(
        functools.partial(write_kernel, sources, cq, pieces),
        out_shape=(
            jax.ShapeDtypeStruct((nq, tall * cq, 128), jnp.float32),
            jax.ShapeDtypeStruct(rest.shape, jnp.float32),
        ),
        in_specs=[
            pl.BlockSpec(memory_space=pltpu.VMEM),
            pl.BlockSpec(memory_space=pltpu.VMEM),
            pl.BlockSpec(memory_space=pltpu.VMEM),
            pl.BlockSpec(memory_space=pltpu.HBM),
        ],
        out_specs=(
            pl.BlockSpec(memory_space=pltpu.HBM),
            pl.BlockSpec(memory_space=pltpu.VMEM),
        ),
        input_output_aliases={1: 1},
        scratch_shapes=[
            pltpu.SMEM((sources,), jnp.int32),
            pltpu.SemaphoreType.DMA,
            pltpu.SemaphoreType.DMA,
        ],
        compiler_params=pltpu.CompilerParams(vmem_limit_bytes=16 * 1024 * 1024),
        name="writing",
    )(head, rest, landed, cells)
    return result.reshape(boundary_block.shape)


def solution(mesh):
    return jax.shard_map(
        functools.partial(on_device, mesh.shape["row"], mesh.shape["col"]),
        mesh=mesh,
        in_specs=(
            P(),
            P(),
            P(("row", "col"), None),
            P(("row", "col"), None),
            P(None, "row", None, "col"),
        ),
        out_specs=P(None, "row", None, "col"),
        check_vma=False,
    )
```

```python
import functools

import jax
import jax.numpy as jnp
from jax import lax
from jax.experimental import pallas as pl
from jax.experimental.pallas import tpu as pltpu
from jax.sharding import PartitionSpec as P

CS = 2
MESH = pl.DeviceIdType.MESH


def around(rows, row_at, at, i):
    fourth = rows // 4
    place = lax.rem(row_at, fourth)
    pair = lax.rem(place // 2 + i // 2, fourth // 2)
    return at * fourth + 2 * pair + lax.rem(place + i, 2)


def is_inner(rows, row_at):
    plane = row_at // (rows // 4)
    return (plane == 1) | (plane == 2)


def exchange_kernel(
    rows, cols, members, slots, width, nq, cq, split,
    listed_ids_ref, listed_counts_ref, factor_ref, couple_ref, boundary_ref,
    head_ref, rest_ref, recv_ref, late_ref, cells_ref,
    ids_ref, counts_ref, w_ref, k_ref, y_ref, p_ref, send_ref, given_ref, cell_ref,
    list_sem, load_sem, send_sem, recv_sem, given_sem, cell_sem, ready_sem,
):
    row_at = lax.axis_index("row")
    col_at = lax.axis_index("col")
    half = rows // 2
    side = row_at // half
    fourth = rows // 4
    plane = row_at // fourth
    inner = is_inner(rows, row_at)
    sides = (0, 1) if cols == 2 else (0, 1, cols - 1)
    sources = CS * rows
    within = functools.partial(around, rows, row_at)

    lists = (
        pltpu.make_async_copy(listed_ids_ref, ids_ref, list_sem.at[0]),
        pltpu.make_async_copy(listed_counts_ref, counts_ref, list_sem.at[1]),
    )
    for load in lists:
        load.start()
    loads = []
    for m in range(members):
        loads.append([pltpu.make_async_copy(factor_ref.at[m], w_ref.at[m], load_sem.at[m, slots])])
        for k in range(slots):
            loads[m].append(
                pltpu.make_async_copy(
                    couple_ref.at[m, :, pl.ds(k * 128, 128)],
                    k_ref[m].at[k],
                    load_sem.at[m, k],
                )
            )
        for load in loads[m]:
            load.start()

    barrier = pltpu.get_barrier_semaphore()
    for hop in range(4):
        for j in sides:
            if hop or j:
                pl.semaphore_signal(
                    barrier, inc=1,
                    device_id=(
                        lax.rem(row_at + hop * fourth, rows), lax.rem(col_at + j, cols)
                    ),
                    device_id_type=MESH,
                )
    for i in range(1, fourth):
        pl.semaphore_signal(
            barrier, inc=1, device_id=(within(plane, i), col_at), device_id_type=MESH
        )

    far_mid = 2 - side

    @pl.when(inner)
    def _():
        for i in range(fourth):
            for j in range(CS):
                at = (j * rows + within(far_mid, i)) * 128
                recv_ref[pl.ds(at, 128)] = jnp.zeros((128, 128), jnp.float32)

    def columns(m, k):
        return jnp.concatenate([k_ref[m][k], k_ref[m][k + 1]], axis=1)

    own = (row_at * cols + col_at) * members
    ends = [within(3 * (1 - side), i) for i in range(fourth)]
    middles = [within(far_mid, i) for i in range(fourth)]
    mates = [within(side * 2 + 1 - lax.rem(plane, 2), i) for i in range(fourth)]
    near = [within(plane, i) for i in range(1, fourth)]
    early = 2
    outer_order = [mates[0], middles[0]]
    for i in range(len(near)):
        outer_order += [mates[i + 1], near[i]]
    outer_order += middles[1:] + ends
    inner_order = [ends[0], mates[0]] + ends[1:]
    for i in range(len(near)):
        inner_order += [mates[i + 1], near[i]]
    inner_order += middles
    targets = [jnp.where(inner, a, b) for a, b in zip(inner_order, outer_order)] + [row_at]
    late = rows - 1 - fourth

    def staged(i, j):
        if late <= i < rows - 1:
            return late_ref, ((i - late) * CS + j) * 128
        return send_ref, (j * rows + i) * 128

    def route(i, target, j):
        ref, at = staged(i, j)
        src = ref.at[pl.ds(at, 128)]
        dst = recv_ref.at[pl.ds((j * rows + row_at) * 128, 128)]
        if j == 0 and i == rows - 1:
            return pltpu.make_async_copy(src, dst, recv_sem)
        return pltpu.make_async_remote_copy(
            src_ref=src,
            dst_ref=dst,
            send_sem=send_sem,
            recv_sem=recv_sem,
            device_id=(target, lax.rem(col_at + j, cols)),
            device_id_type=MESH,
        )

    def launch(i):
        for j in range(CS):
            route(i, targets[i], j).start()

    def pick(target):
        picks = []
        for m in range(members):
            k, weight = jnp.int32(0), jnp.float32(0.0)
            count = counts_ref[own + m]
            for kk in range(slots):
                hit = (lax.rem(ids_ref[kk, own + m], rows) == target) & (kk < count)
                k = jnp.where(hit, jnp.int32(kk), k)
                weight = jnp.where(hit, jnp.float32(1.0), weight)
            picks.append((k, weight))
        return picks

    for load in lists:
        load.wait()
    merged = 1
    picked = [pick(targets[i]) for i in range(early)]
    parts = []
    for m in range(members):
        for load in loads[m]:
            load.wait()
        blocks = [k_ref[m][k] for k in range(CS)]
        blocks += [k_ref[m][picked[i][m][0]] for i in range(merged)]
        made = jnp.dot(
            w_ref[m], jnp.concatenate(blocks, axis=1), preferred_element_type=jnp.float32
        ).astype(jnp.bfloat16)
        y_ref[m, :, 0 : CS * 128] = made[:, 0 : CS * 128]
        parts.append(
            lax.dot_general(
                made[:, CS * 128 :],
                made[:, 0 : CS * 128],
                (((0,), (0,)), ((), ())),
                preferred_element_type=jnp.float32,
            )
        )
    for i in range(early):
        if i >= merged:
            made = []
            for m in range(members):
                block = jnp.dot(
                    w_ref[m], k_ref[m][picked[i][m][0]], preferred_element_type=jnp.float32
                ).astype(jnp.bfloat16)
                made.append(
                    lax.dot_general(
                        block,
                        y_ref[m, :, 0 : CS * 128],
                        (((0,), (0,)), ((), ())),
                        preferred_element_type=jnp.float32,
                    )
                )
        else:
            made = [part[i * 128 : (i + 1) * 128] for part in parts]
        total = made[0] * picked[i][0][1]
        for m in range(1, members):
            total = total + made[m] * picked[i][m][1]
        for j in range(CS):
            send_ref[(j * rows + i) * 128 : (j * rows + i + 1) * 128] = total[
                :, j * 128 : (j + 1) * 128
            ]
        if i == 0:
            pl.semaphore_wait(barrier, 4 * len(sides) - 1 + fourth - 1)
            for n in range(1, fourth):
                pl.semaphore_signal(
                    ready_sem, inc=1, device_id=(within(plane, n), col_at), device_id_type=MESH
                )
        launch(i)
        if i == 0:
            given = pltpu.make_async_copy(boundary_ref, given_ref, given_sem)
            given.start()

    for m in range(members):
        for n in range(CS * 128, slots * 128, 256):
            y_ref[m, :, n : n + 256] = jnp.dot(
                w_ref[m], columns(m, n // 128), preferred_element_type=jnp.float32
            ).astype(jnp.bfloat16)
        for n in range(0, slots, 2):
            part = lax.dot_general(
                y_ref[m, :, n * 128 : n * 128 + 256],
                y_ref[m, :, 0 : CS * 128],
                (((0,), (0,)), ((), ())),
                preferred_element_type=jnp.float32,
            )
            for d in range(2):
                for j in range(CS):
                    p_ref[m * slots + n + d, j] = part[
                        d * 128 : (d + 1) * 128, j * 128 : (j + 1) * 128
                    ]

    for i in range(early, rows):
        picks = pick(targets[i])
        for j in range(CS):
            total = p_ref[picks[0][0], j] * picks[0][1]
            for m in range(1, members):
                total = total + p_ref[m * slots + picks[m][0], j] * picks[m][1]
            ref, at = staged(i, j)
            ref[at : at + 128] = total
        if i == early:
            pl.semaphore_wait(ready_sem, fourth - 1)
        elif i <= late:
            launch(i - 1)
    launch(rows - 1)

    @pl.when(jnp.logical_not(inner))
    def _():
        for i in range(late, rows - 1):
            launch(i)

    def add_source(r, carry):
        for j in range(CS):
            first = (r * cols + lax.rem(col_at + cols - j, cols)) * members
            cell = jnp.int32(0)
            column = lax.div(ids_ref[j, first], cols)
            for m in range(members):
                for kk in range(slots):
                    if m > 0 and kk < CS:
                        continue
                    ident = ids_ref[kk, first + m]
                    cell = jnp.where(
                        lax.rem(ident, rows) == row_at,
                        lax.div(ident, rows) * cq + column,
                        cell,
                    )
            cell_ref[j * rows + r] = cell
        return carry

    lax.fori_loop(0, rows, add_source, 0)
    for i in range(fourth):
        for j in range(CS):
            cell_ref[sources + i * CS + j] = cell_ref[j * rows + within(far_mid, i)]
    listed = pltpu.make_async_copy(cell_ref, cells_ref, cell_sem)
    listed.start()

    given.wait()
    tall = given_ref.shape[1]

    def widen(q, carry):
        head_ref[q] = given_ref[q, :split].astype(jnp.float32).reshape(split * cq, 128)
        rest_ref[q] = given_ref[q, split:].astype(jnp.float32).reshape((tall - split) * cq, 128)
        return carry

    lax.fori_loop(0, nq, widen, 0)
    listed.wait()

    def settled(tiles):
        arrived = recv_ref.at[pl.ds(0, tiles * 128)]
        pltpu.make_async_copy(arrived, arrived, recv_sem).wait()
        sent = send_ref.at[pl.ds(0, (tiles - 1) * 128)]
        pltpu.make_async_copy(sent, sent, send_sem).wait()

    @pl.when(inner)
    def _():
        settled(sources - fourth * CS)

    @pl.when(jnp.logical_not(inner))
    def _():
        settled(sources)


def write_kernel(
    sources, cq, split,
    head_in_ref, rest_in_ref, recv_ref, cells_ref,
    out_ref, head_ref, rest_ref,
    cell_ref, cell_sem, sem,
):
    listed = pltpu.make_async_copy(cells_ref, cell_ref, cell_sem)
    listed.start()
    listed.wait()
    nq = head_ref.shape[0]
    tall = out_ref.shape[1] // cq

    for ref, start, height in ((head_ref, 0, split), (rest_ref, split, tall - split)):

        def settle(s, carry):
            cell = cell_ref[s]
            at = (lax.div(cell, cq), pl.ds(lax.rem(cell, cq), height, stride=cq), slice(None))
            ref[at] = ref[at] - recv_ref[pl.ds(pl.multiple_of(s * 128, 128) + start, height)]
            return carry

        lax.fori_loop(0, sources, settle, 0)
        for q in range(nq):
            pltpu.make_async_copy(
                ref.at[q], out_ref.at[q, pl.ds(start * cq, height * cq)], sem
            ).start()
    pltpu.make_async_copy(out_ref, out_ref, sem).wait()


def late_kernel(rows, cols, late_ref, after_ref, recv_ref, send_sem, recv_sem):
    row_at = lax.axis_index("row")
    col_at = lax.axis_index("col")
    sides = (0, 1) if cols == 2 else (0, 1, cols - 1)
    barrier = pltpu.get_barrier_semaphore()
    partners = [around(rows, row_at, 2 - row_at // (rows // 2), i) for i in range((rows // 4))]

    @pl.when(is_inner(rows, row_at))
    def _():
        for partner in partners:
            for j in sides:
                pl.semaphore_signal(
                    barrier, inc=1, device_id=(partner, lax.rem(col_at + j, cols)),
                    device_id_type=MESH,
                )
        pl.semaphore_wait(barrier, (rows // 4) * len(sides))
        for i, partner in enumerate(partners):
            for j in range(CS):
                part = pl.ds((i * CS + j) * 128, 128)
                pltpu.make_async_remote_copy(
                    src_ref=late_ref.at[part],
                    dst_ref=recv_ref.at[part],
                    send_sem=send_sem,
                    recv_sem=recv_sem,
                    device_id=(partner, lax.rem(col_at + j, cols)),
                    device_id_type=MESH,
                ).start()
        pltpu.make_async_copy(recv_ref, recv_ref, recv_sem).wait()
        pltpu.make_async_copy(late_ref, late_ref, send_sem).wait()


def patch_kernel(
    rows, sources, cq, split,
    result_ref, head_in_ref, rest_in_ref, recv_ref, cells_ref,
    out_ref, head_ref, rest_ref,
    cell_ref, cell_sem, sem,
):
    tall = out_ref.shape[1] // cq
    parts = ((head_ref, 0, split), (rest_ref, split, tall - split))

    @pl.when(is_inner(rows, lax.axis_index("row")))
    def _():
        listed = pltpu.make_async_copy(cells_ref, cell_ref, cell_sem)
        listed.start()
        listed.wait()
        cells = [cell_ref[sources + n] for n in range((rows // 4) * CS)]
        for n, cell in enumerate(cells):
            for ref, start, height in parts:
                at = (lax.div(cell, cq), pl.ds(lax.rem(cell, cq), height, stride=cq), slice(None))
                ref[at] = ref[at] - recv_ref[n * 128 + start : n * 128 + start + height]
        copies = []
        for cell in cells:
            q = lax.div(cell, cq)
            for ref, start, height in parts:
                copies.append(
                    pltpu.make_async_copy(
                        ref.at[q], out_ref.at[q, pl.ds(start * cq, height * cq)], sem
                    )
                )
                copies[-1].start()
        for copy in copies:
            copy.wait()


def kept(value):
    return pltpu.with_memory_space_constraint(value, pltpu.HBM)


def on_device(rows, cols, block_ids, iface_counts, inv_factor, coupling, boundary_block):
    slots = block_ids.shape[1]
    width = inv_factor.shape[1]
    members = inv_factor.shape[0] // width
    nq, tall, cq, _ = boundary_block.shape
    sources = CS * rows
    split = 48
    vmem = pl.BlockSpec(memory_space=pltpu.VMEM)
    hbm = pl.BlockSpec(memory_space=pltpu.HBM)
    head_shape = jax.ShapeDtypeStruct((nq, split * cq, 128), jnp.float32)
    rest_shape = jax.ShapeDtypeStruct((nq, (tall - split) * cq, 128), jnp.float32)
    late_shape = jax.ShapeDtypeStruct(((rows // 4) * CS * 128, 128), jnp.float32)
    result_shape = jax.ShapeDtypeStruct((nq, tall * cq, 128), jnp.float32)
    head, rest, landed, late, cells = pl.pallas_call(
        functools.partial(exchange_kernel, rows, cols, members, slots, width, nq, cq, split),
        out_shape=(
            head_shape,
            rest_shape,
            jax.ShapeDtypeStruct((sources * 128, 128), jnp.float32),
            late_shape,
            jax.ShapeDtypeStruct((sources + (rows // 4) * CS,), jnp.int32),
        ),
        in_specs=[hbm] * 5,
        out_specs=(vmem, vmem, vmem, vmem, hbm),
        scratch_shapes=[
            pltpu.SMEM((slots, block_ids.shape[0]), jnp.int32),
            pltpu.SMEM((block_ids.shape[0],), jnp.int32),
            pltpu.VMEM((members, width, width), jnp.bfloat16),
            [pltpu.VMEM((slots, width, 128), jnp.bfloat16)] * members,
            pltpu.VMEM((members, width, slots * 128), jnp.bfloat16),
            pltpu.VMEM((members * slots, CS, 128, 128), jnp.float32),
            pltpu.VMEM((sources * 128, 128), jnp.float32),
            pltpu.VMEM(boundary_block.shape, jnp.bfloat16),
            pltpu.SMEM((sources + (rows // 4) * CS,), jnp.int32),
            pltpu.SemaphoreType.DMA((2,)),
            pltpu.SemaphoreType.DMA((members, slots + 1)),
            pltpu.SemaphoreType.DMA,
            pltpu.SemaphoreType.DMA,
            pltpu.SemaphoreType.DMA,
            pltpu.SemaphoreType.DMA,
            pltpu.SemaphoreType.REGULAR,
        ],
        compiler_params=pltpu.CompilerParams(
            collective_id=0, has_side_effects=True, vmem_limit_bytes=32 * 1024 * 1024
        ),
        name="exchange",
    )(
        kept(block_ids.T),
        kept(iface_counts),
        kept(inv_factor.reshape(members, width, width)),
        kept(coupling.reshape(members, width, slots * 128)),
        kept(boundary_block),
    )
    local = [
        pltpu.SMEM((sources + (rows // 4) * CS,), jnp.int32),
        pltpu.SemaphoreType.DMA,
        pltpu.SemaphoreType.DMA,
    ]
    result, head, rest = pl.pallas_call(
        functools.partial(write_kernel, sources, cq, split),
        out_shape=(result_shape, head_shape, rest_shape),
        in_specs=[vmem, vmem, vmem, hbm],
        out_specs=(hbm, vmem, vmem),
        input_output_aliases={0: 1, 1: 2},
        scratch_shapes=local,
        compiler_params=pltpu.CompilerParams(vmem_limit_bytes=16 * 1024 * 1024),
        name="writing",
    )(head, rest, landed, cells)
    landed = pl.pallas_call(
        functools.partial(late_kernel, rows, cols),
        out_shape=late_shape,
        in_specs=[vmem, vmem],
        out_specs=vmem,
        scratch_shapes=[pltpu.SemaphoreType.DMA, pltpu.SemaphoreType.DMA],
        compiler_params=pltpu.CompilerParams(
            collective_id=1, has_side_effects=True, vmem_limit_bytes=16 * 1024 * 1024
        ),
        name="late",
    )(late, rest)
    result, _, _ = pl.pallas_call(
        functools.partial(patch_kernel, rows, sources, cq, split),
        out_shape=(result_shape, head_shape, rest_shape),
        in_specs=[hbm, vmem, vmem, vmem, hbm],
        out_specs=(hbm, vmem, vmem),
        input_output_aliases={0: 0, 1: 1, 2: 2},
        scratch_shapes=local,
        compiler_params=pltpu.CompilerParams(vmem_limit_bytes=16 * 1024 * 1024),
        name="patching",
    )(result, head, rest, landed, cells)
    return result.reshape(boundary_block.shape)


def solution(mesh):
    return jax.shard_map(
        functools.partial(on_device, mesh.shape["row"], mesh.shape["col"]),
        mesh=mesh,
        in_specs=(
            P(),
            P(),
            P(("row", "col"), None),
            P(("row", "col"), None),
            P(None, "row", None, "col"),
        ),
        out_specs=P(None, "row", None, "col"),
        check_vma=False,
    )
```

```python
import functools

import jax
import jax.numpy as jnp
from jax import lax
from jax.experimental import pallas as pl
from jax.experimental.pallas import tpu as pltpu
from jax.sharding import PartitionSpec as P

CS = 2
MESH = pl.DeviceIdType.MESH


def around(rows, row_at, at, i):
    fourth = rows // 4
    place = lax.rem(row_at, fourth)
    pair = lax.rem(place // 2 + i // 2, fourth // 2)
    return at * fourth + 2 * pair + lax.rem(place + i, 2)


def is_inner(rows, row_at):
    plane = row_at // (rows // 4)
    return (plane == 1) | (plane == 2)


def exchange_kernel(
    rows, cols, members, slots, width, nq, cq, split,
    listed_ids_ref, listed_counts_ref, factor_ref, couple_ref, boundary_ref,
    head_ref, rest_ref, recv_ref, late_ref, cells_ref,
    ids_ref, counts_ref, w_ref, k_ref, y_ref, p_ref, send_ref, given_ref, cell_ref,
    list_sem, load_sem, send_sem, recv_sem, given_sem, cell_sem, ready_sem,
):
    row_at = lax.axis_index("row")
    col_at = lax.axis_index("col")
    half = rows // 2
    side = row_at // half
    fourth = rows // 4
    plane = row_at // fourth
    inner = is_inner(rows, row_at)
    sides = (0, 1) if cols == 2 else (0, 1, cols - 1)
    sources = CS * rows
    within = functools.partial(around, rows, row_at)

    lists = (
        pltpu.make_async_copy(listed_ids_ref, ids_ref, list_sem.at[0]),
        pltpu.make_async_copy(listed_counts_ref, counts_ref, list_sem.at[1]),
    )
    for load in lists:
        load.start()
    loads = []
    for m in range(members):
        loads.append([pltpu.make_async_copy(factor_ref.at[m], w_ref.at[m], load_sem.at[m, slots])])
        for k in range(slots):
            loads[m].append(
                pltpu.make_async_copy(
                    couple_ref.at[m, :, pl.ds(k * 128, 128)],
                    k_ref[m].at[k],
                    load_sem.at[m, k],
                )
            )
        for load in loads[m]:
            load.start()

    far_end, far_mid, mate = 3 * (1 - side), 2 - side, side * 2 + 1 - lax.rem(plane, 2)
    barrier = pltpu.get_barrier_semaphore()

    def greet(at, i, j):
        pl.semaphore_signal(
            barrier, inc=1, device_id=(within(at, i), lax.rem(col_at + j, cols)),
            device_id_type=MESH,
        )

    for j in sides:
        greet(mate, 0, j)
        greet(far_mid, 0, j)
        if j:
            greet(plane, 0, j)

    @pl.when(inner)
    def _():
        for j in sides:
            greet(far_end, 0, j)
        for i in range(1, fourth):
            greet(plane, i, 0)

    @pl.when(inner)
    def _():
        for i in range(fourth):
            for j in range(CS):
                at = (j * rows + within(far_mid, i)) * 128
                recv_ref[pl.ds(at, 128)] = jnp.zeros((128, 128), jnp.float32)

    def columns(m, k):
        return jnp.concatenate([k_ref[m][k], k_ref[m][k + 1]], axis=1)

    own = (row_at * cols + col_at) * members
    ends = [within(far_end, i) for i in range(fourth)]
    middles = [within(far_mid, i) for i in range(fourth)]
    mates = [within(mate, i) for i in range(fourth)]
    near = [within(plane, i) for i in range(1, fourth)]
    early = 2
    outer_order = [mates[0], middles[0]]
    for i in range(1, fourth - 1):
        outer_order += [mates[i], near[i - 1]]
    outer_order += middles[1:] + [mates[-1], near[-1]] + ends
    inner_order = [ends[0], mates[0]] + ends[1:] + near + mates[1:]
    inner_order += middles
    targets = [jnp.where(inner, a, b) for a, b in zip(inner_order, outer_order)] + [row_at]
    late = rows - 1 - fourth

    def staged(i, j):
        if late <= i < rows - 1:
            return late_ref, ((i - late) * CS + j) * 128
        return send_ref, (j * rows + i) * 128

    def route(i, target, j):
        ref, at = staged(i, j)
        src = ref.at[pl.ds(at, 128)]
        dst = recv_ref.at[pl.ds((j * rows + row_at) * 128, 128)]
        if j == 0 and i == rows - 1:
            return pltpu.make_async_copy(src, dst, recv_sem)
        return pltpu.make_async_remote_copy(
            src_ref=src,
            dst_ref=dst,
            send_sem=send_sem,
            recv_sem=recv_sem,
            device_id=(target, lax.rem(col_at + j, cols)),
            device_id_type=MESH,
        )

    def launch(i):
        for j in range(CS):
            route(i, targets[i], j).start()

    def pick(target):
        picks = []
        for m in range(members):
            k, weight = jnp.int32(0), jnp.float32(0.0)
            count = counts_ref[own + m]
            for kk in range(slots):
                hit = (lax.rem(ids_ref[kk, own + m], rows) == target) & (kk < count)
                k = jnp.where(hit, jnp.int32(kk), k)
                weight = jnp.where(hit, jnp.float32(1.0), weight)
            picks.append((k, weight))
        return picks

    for load in lists:
        load.wait()
    merged = 1
    picked = [pick(targets[i]) for i in range(early)]
    parts = []
    for m in range(members):
        for load in loads[m]:
            load.wait()
        blocks = [k_ref[m][k] for k in range(CS)]
        blocks += [k_ref[m][picked[i][m][0]] for i in range(merged)]
        made = jnp.dot(
            w_ref[m], jnp.concatenate(blocks, axis=1), preferred_element_type=jnp.float32
        ).astype(jnp.bfloat16)
        y_ref[m, :, 0 : CS * 128] = made[:, 0 : CS * 128]
        parts.append(
            lax.dot_general(
                made[:, CS * 128 :],
                made[:, 0 : CS * 128],
                (((0,), (0,)), ((), ())),
                preferred_element_type=jnp.float32,
            )
        )
    for i in range(early):
        if i >= merged:
            made = []
            for m in range(members):
                block = jnp.dot(
                    w_ref[m], k_ref[m][picked[i][m][0]], preferred_element_type=jnp.float32
                ).astype(jnp.bfloat16)
                made.append(
                    lax.dot_general(
                        block,
                        y_ref[m, :, 0 : CS * 128],
                        (((0,), (0,)), ((), ())),
                        preferred_element_type=jnp.float32,
                    )
                )
        else:
            made = [part[i * 128 : (i + 1) * 128] for part in parts]
        total = made[0] * picked[i][0][1]
        for m in range(1, members):
            total = total + made[m] * picked[i][m][1]
        for j in range(CS):
            send_ref[(j * rows + i) * 128 : (j * rows + i + 1) * 128] = total[
                :, j * 128 : (j + 1) * 128
            ]
        if i == 0:
            met = 3 * len(sides) - 1
            pl.semaphore_wait(barrier, jnp.where(inner, met + len(sides) + fourth - 1, met))

            @pl.when(inner)
            def _():
                for n in range(1, fourth):
                    pl.semaphore_signal(
                        ready_sem, inc=1, device_id=(within(plane, n), col_at), device_id_type=MESH
                    )

        launch(i)
        if i == 0:
            given = pltpu.make_async_copy(boundary_ref, given_ref, given_sem)
            given.start()

    for m in range(members):
        for n in range(CS * 128, slots * 128, 256):
            y_ref[m, :, n : n + 256] = jnp.dot(
                w_ref[m], columns(m, n // 128), preferred_element_type=jnp.float32
            ).astype(jnp.bfloat16)
        for n in range(0, slots, 2):
            part = lax.dot_general(
                y_ref[m, :, n * 128 : n * 128 + 256],
                y_ref[m, :, 0 : CS * 128],
                (((0,), (0,)), ((), ())),
                preferred_element_type=jnp.float32,
            )
            for d in range(2):
                for j in range(CS):
                    p_ref[m * slots + n + d, j] = part[
                        d * 128 : (d + 1) * 128, j * 128 : (j + 1) * 128
                    ]

    for i in range(early, rows):
        picks = pick(targets[i])
        for j in range(CS):
            total = p_ref[picks[0][0], j] * picks[0][1]
            for m in range(1, members):
                total = total + p_ref[m * slots + picks[m][0], j] * picks[m][1]
            ref, at = staged(i, j)
            ref[at : at + 128] = total
        if i == early:
            pl.semaphore_wait(ready_sem, jnp.where(inner, fourth - 1, 1))

            @pl.when(inner)
            def _():
                pl.semaphore_signal(
                    ready_sem, inc=1, device_id=(within(mate, 0), col_at), device_id_type=MESH
                )

        elif i <= late:
            launch(i - 1)
    launch(rows - 1)

    @pl.when(jnp.logical_not(inner))
    def _():
        for i in range(late, rows - 1):
            launch(i)

    def add_source(r, carry):
        for j in range(CS):
            first = (r * cols + lax.rem(col_at + cols - j, cols)) * members
            cell = jnp.int32(0)
            column = lax.div(ids_ref[j, first], cols)
            for m in range(members):
                for kk in range(slots):
                    if m > 0 and kk < CS:
                        continue
                    ident = ids_ref[kk, first + m]
                    cell = jnp.where(
                        lax.rem(ident, rows) == row_at,
                        lax.div(ident, rows) * cq + column,
                        cell,
                    )
            cell_ref[j * rows + r] = cell
        return carry

    lax.fori_loop(0, rows, add_source, 0)
    for i in range(fourth):
        for j in range(CS):
            cell_ref[sources + i * CS + j] = cell_ref[j * rows + within(far_mid, i)]
    listed = pltpu.make_async_copy(cell_ref, cells_ref, cell_sem)
    listed.start()

    given.wait()
    tall = given_ref.shape[1]

    def widen(q, carry):
        head_ref[q] = given_ref[q, :split].astype(jnp.float32).reshape(split * cq, 128)
        rest_ref[q] = given_ref[q, split:].astype(jnp.float32).reshape((tall - split) * cq, 128)
        return carry

    lax.fori_loop(0, nq, widen, 0)
    listed.wait()

    def settled(tiles):
        arrived = recv_ref.at[pl.ds(0, tiles * 128)]
        pltpu.make_async_copy(arrived, arrived, recv_sem).wait()
        sent = send_ref.at[pl.ds(0, (tiles - 1) * 128)]
        pltpu.make_async_copy(sent, sent, send_sem).wait()

    @pl.when(inner)
    def _():
        settled(sources - fourth * CS)

    @pl.when(jnp.logical_not(inner))
    def _():
        settled(sources)


def write_kernel(
    sources, cq, split,
    head_in_ref, rest_in_ref, recv_ref, cells_ref,
    out_ref, head_ref, rest_ref,
    cell_ref, cell_sem, sem,
):
    listed = pltpu.make_async_copy(cells_ref, cell_ref, cell_sem)
    listed.start()
    listed.wait()
    nq = head_ref.shape[0]
    tall = out_ref.shape[1] // cq

    for ref, start, height in ((head_ref, 0, split), (rest_ref, split, tall - split)):

        def settle(s, carry):
            cell = cell_ref[s]
            at = (lax.div(cell, cq), pl.ds(lax.rem(cell, cq), height, stride=cq), slice(None))
            ref[at] = ref[at] - recv_ref[pl.ds(pl.multiple_of(s * 128, 128) + start, height)]
            return carry

        lax.fori_loop(0, sources, settle, 0)
        for q in range(nq):
            pltpu.make_async_copy(
                ref.at[q], out_ref.at[q, pl.ds(start * cq, height * cq)], sem
            ).start()
    pltpu.make_async_copy(out_ref, out_ref, sem).wait()


def late_kernel(rows, cols, late_ref, after_ref, recv_ref, send_sem, recv_sem):
    row_at = lax.axis_index("row")
    col_at = lax.axis_index("col")
    sides = (0, 1) if cols == 2 else (0, 1, cols - 1)
    barrier = pltpu.get_barrier_semaphore()
    partners = [around(rows, row_at, 2 - row_at // (rows // 2), i) for i in range((rows // 4))]

    @pl.when(is_inner(rows, row_at))
    def _():
        for partner in partners:
            for j in sides:
                pl.semaphore_signal(
                    barrier, inc=1, device_id=(partner, lax.rem(col_at + j, cols)),
                    device_id_type=MESH,
                )
        pl.semaphore_wait(barrier, (rows // 4) * len(sides))
        for i, partner in enumerate(partners):
            for j in range(CS):
                part = pl.ds((i * CS + j) * 128, 128)
                pltpu.make_async_remote_copy(
                    src_ref=late_ref.at[part],
                    dst_ref=recv_ref.at[part],
                    send_sem=send_sem,
                    recv_sem=recv_sem,
                    device_id=(partner, lax.rem(col_at + j, cols)),
                    device_id_type=MESH,
                ).start()
        pltpu.make_async_copy(recv_ref, recv_ref, recv_sem).wait()
        pltpu.make_async_copy(late_ref, late_ref, send_sem).wait()


def patch_kernel(
    rows, sources, cq, split,
    result_ref, head_in_ref, rest_in_ref, recv_ref, cells_ref,
    out_ref, head_ref, rest_ref,
    sem,
):
    tall = out_ref.shape[1] // cq
    parts = ((head_ref, 0, split), (rest_ref, split, tall - split))

    @pl.when(is_inner(rows, lax.axis_index("row")))
    def _():
        listed = cells_ref[...]
        lane = lax.broadcasted_iota(jnp.int32, listed.shape, 0)
        cells = [
            jnp.sum(jnp.where(lane == sources + n, listed, 0)) for n in range((rows // 4) * CS)
        ]
        for n, cell in enumerate(cells):
            for ref, start, height in parts:
                at = (lax.div(cell, cq), pl.ds(lax.rem(cell, cq), height, stride=cq), slice(None))
                ref[at] = ref[at] - recv_ref[n * 128 + start : n * 128 + start + height]
        copies = []
        for cell in cells:
            q = lax.div(cell, cq)
            for ref, start, height in parts:
                copies.append(
                    pltpu.make_async_copy(
                        ref.at[q], out_ref.at[q, pl.ds(start * cq, height * cq)], sem
                    )
                )
                copies[-1].start()
        for copy in copies:
            copy.wait()


def kept(value):
    return pltpu.with_memory_space_constraint(value, pltpu.HBM)


def on_device(rows, cols, block_ids, iface_counts, inv_factor, coupling, boundary_block):
    slots = block_ids.shape[1]
    width = inv_factor.shape[1]
    members = inv_factor.shape[0] // width
    nq, tall, cq, _ = boundary_block.shape
    sources = CS * rows
    split = 48
    vmem = pl.BlockSpec(memory_space=pltpu.VMEM)
    hbm = pl.BlockSpec(memory_space=pltpu.HBM)
    head_shape = jax.ShapeDtypeStruct((nq, split * cq, 128), jnp.float32)
    rest_shape = jax.ShapeDtypeStruct((nq, (tall - split) * cq, 128), jnp.float32)
    late_shape = jax.ShapeDtypeStruct(((rows // 4) * CS * 128, 128), jnp.float32)
    result_shape = jax.ShapeDtypeStruct((nq, tall * cq, 128), jnp.float32)
    head, rest, landed, late, cells = pl.pallas_call(
        functools.partial(exchange_kernel, rows, cols, members, slots, width, nq, cq, split),
        out_shape=(
            head_shape,
            rest_shape,
            jax.ShapeDtypeStruct((sources * 128, 128), jnp.float32),
            late_shape,
            jax.ShapeDtypeStruct((sources + (rows // 4) * CS,), jnp.int32),
        ),
        in_specs=[hbm] * 5,
        out_specs=(vmem, vmem, vmem, vmem, hbm),
        scratch_shapes=[
            pltpu.SMEM((slots, block_ids.shape[0]), jnp.int32),
            pltpu.SMEM((block_ids.shape[0],), jnp.int32),
            pltpu.VMEM((members, width, width), jnp.bfloat16),
            [pltpu.VMEM((slots, width, 128), jnp.bfloat16)] * members,
            pltpu.VMEM((members, width, slots * 128), jnp.bfloat16),
            pltpu.VMEM((members * slots, CS, 128, 128), jnp.float32),
            pltpu.VMEM((sources * 128, 128), jnp.float32),
            pltpu.VMEM(boundary_block.shape, jnp.bfloat16),
            pltpu.SMEM((sources + (rows // 4) * CS,), jnp.int32),
            pltpu.SemaphoreType.DMA((2,)),
            pltpu.SemaphoreType.DMA((members, slots + 1)),
            pltpu.SemaphoreType.DMA,
            pltpu.SemaphoreType.DMA,
            pltpu.SemaphoreType.DMA,
            pltpu.SemaphoreType.DMA,
            pltpu.SemaphoreType.REGULAR,
        ],
        compiler_params=pltpu.CompilerParams(
            collective_id=0, has_side_effects=True, vmem_limit_bytes=32 * 1024 * 1024
        ),
        name="exchange",
    )(
        kept(block_ids.T),
        kept(iface_counts),
        kept(inv_factor.reshape(members, width, width)),
        kept(coupling.reshape(members, width, slots * 128)),
        kept(boundary_block),
    )
    local = [
        pltpu.SMEM((sources + (rows // 4) * CS,), jnp.int32),
        pltpu.SemaphoreType.DMA,
        pltpu.SemaphoreType.DMA,
    ]
    result, head, rest = pl.pallas_call(
        functools.partial(write_kernel, sources, cq, split),
        out_shape=(result_shape, head_shape, rest_shape),
        in_specs=[vmem, vmem, vmem, hbm],
        out_specs=(hbm, vmem, vmem),
        input_output_aliases={0: 1, 1: 2},
        scratch_shapes=local,
        compiler_params=pltpu.CompilerParams(vmem_limit_bytes=16 * 1024 * 1024),
        name="writing",
    )(head, rest, landed, cells)
    landed = pl.pallas_call(
        functools.partial(late_kernel, rows, cols),
        out_shape=late_shape,
        in_specs=[vmem, vmem],
        out_specs=vmem,
        scratch_shapes=[pltpu.SemaphoreType.DMA, pltpu.SemaphoreType.DMA],
        compiler_params=pltpu.CompilerParams(
            collective_id=1, has_side_effects=True, vmem_limit_bytes=16 * 1024 * 1024
        ),
        name="late",
    )(late, rest)
    result, _, _ = pl.pallas_call(
        functools.partial(patch_kernel, rows, sources, cq, split),
        out_shape=(result_shape, head_shape, rest_shape),
        in_specs=[hbm, vmem, vmem, vmem, vmem],
        out_specs=(hbm, vmem, vmem),
        input_output_aliases={0: 0, 1: 1, 2: 2},
        scratch_shapes=local[2:],
        compiler_params=pltpu.CompilerParams(vmem_limit_bytes=16 * 1024 * 1024),
        name="patching",
    )(result, head, rest, landed, cells)
    return result.reshape(boundary_block.shape)


def solution(mesh):
    return jax.shard_map(
        functools.partial(on_device, mesh.shape["row"], mesh.shape["col"]),
        mesh=mesh,
        in_specs=(
            P(),
            P(),
            P(("row", "col"), None),
            P(("row", "col"), None),
            P(None, "row", None, "col"),
        ),
        out_specs=P(None, "row", None, "col"),
        check_vma=False,
    )
```

```python
import functools

import jax
import jax.numpy as jnp
from jax import lax
from jax.experimental import pallas as pl
from jax.experimental.pallas import tpu as pltpu
from jax.sharding import PartitionSpec as P

CS = 2
MESH = pl.DeviceIdType.MESH


def around(rows, row_at, at, i):
    fourth = rows // 4
    place = lax.rem(row_at, fourth)
    pair = lax.rem(place // 2 + i // 2, fourth // 2)
    return at * fourth + 2 * pair + lax.rem(place + i, 2)


def is_inner(rows, row_at):
    plane = row_at // (rows // 4)
    return (plane == 1) | (plane == 2)


def exchange_kernel(
    rows, cols, members, slots, width, nq, cq, split,
    listed_ids_ref, listed_counts_ref, factor_ref, couple_ref, boundary_ref,
    head_ref, rest_ref, recv_ref, late_ref, cells_ref,
    ids_ref, counts_ref, w_ref, k_ref, y_ref, p_ref, send_ref, given_ref, cell_ref,
    list_sem, load_sem, send_sem, recv_sem, given_sem, cell_sem, ready_sem,
):
    row_at = lax.axis_index("row")
    col_at = lax.axis_index("col")
    half = rows // 2
    side = row_at // half
    fourth = rows // 4
    plane = row_at // fourth
    inner = is_inner(rows, row_at)
    sides = (0, 1) if cols == 2 else (0, 1, cols - 1)
    sources = CS * rows
    within = functools.partial(around, rows, row_at)

    lists = (
        pltpu.make_async_copy(listed_ids_ref, ids_ref, list_sem.at[0]),
        pltpu.make_async_copy(listed_counts_ref, counts_ref, list_sem.at[1]),
    )
    for load in lists:
        load.start()
    loads = []
    for m in range(members):
        loads.append([pltpu.make_async_copy(factor_ref.at[m], w_ref.at[m], load_sem.at[m, 1])])
        loads[m].append(pltpu.make_async_copy(couple_ref.at[m], k_ref.at[m], load_sem.at[m, 0]))
        for load in loads[m]:
            load.start()

    far_end, far_mid, mate = 3 * (1 - side), 2 - side, side * 2 + 1 - lax.rem(plane, 2)
    barrier = pltpu.get_barrier_semaphore()

    def greet(at, i, j):
        pl.semaphore_signal(
            barrier, inc=1, device_id=(within(at, i), lax.rem(col_at + j, cols)),
            device_id_type=MESH,
        )

    for j in sides:
        greet(mate, 0, j)
        greet(far_mid, 0, j)
        if j:
            greet(plane, 0, j)

    @pl.when(inner)
    def _():
        for j in sides:
            greet(far_end, 0, j)
        for i in range(1, fourth):
            greet(plane, i, 0)

    @pl.when(inner)
    def _():
        for i in range(fourth):
            for j in range(CS):
                at = (j * rows + within(far_mid, i)) * 128
                recv_ref[pl.ds(at, 128)] = jnp.zeros((128, 128), jnp.float32)

    def chosen(m, k):
        block = k_ref[m, :, 0:128]
        for kk in range(1, slots):
            block = jnp.where(k == kk, k_ref[m, :, kk * 128 : kk * 128 + 128], block)
        return block

    def columns(m, k):
        return k_ref[m, :, k * 128 : k * 128 + 256]

    own = (row_at * cols + col_at) * members
    ends = [within(far_end, i) for i in range(fourth)]
    middles = [within(far_mid, i) for i in range(fourth)]
    mates = [within(mate, i) for i in range(fourth)]
    near = [within(plane, i) for i in range(1, fourth)]
    early = 2
    outer_order = [mates[0], middles[0]]
    for i in range(1, fourth - 1):
        outer_order += [mates[i], near[i - 1]]
    outer_order += middles[1:] + [mates[-1], near[-1]] + ends
    inner_order = [ends[0], mates[0]] + ends[1:] + near + mates[1:]
    inner_order += middles
    targets = [jnp.where(inner, a, b) for a, b in zip(inner_order, outer_order)] + [row_at]
    late = rows - 1 - fourth

    def staged(i, j):
        if late <= i < rows - 1:
            return late_ref, ((i - late) * CS + j) * 128
        return send_ref, (j * rows + i) * 128

    def route(i, target, j):
        ref, at = staged(i, j)
        src = ref.at[pl.ds(at, 128)]
        dst = recv_ref.at[pl.ds((j * rows + row_at) * 128, 128)]
        if j == 0 and i == rows - 1:
            return pltpu.make_async_copy(src, dst, recv_sem)
        return pltpu.make_async_remote_copy(
            src_ref=src,
            dst_ref=dst,
            send_sem=send_sem,
            recv_sem=recv_sem,
            device_id=(target, lax.rem(col_at + j, cols)),
            device_id_type=MESH,
        )

    def launch(i):
        for j in range(CS):
            route(i, targets[i], j).start()

    def pick(target):
        picks = []
        for m in range(members):
            k, weight = jnp.int32(0), jnp.float32(0.0)
            count = counts_ref[own + m]
            for kk in range(slots):
                hit = (lax.rem(ids_ref[kk, own + m], rows) == target) & (kk < count)
                k = jnp.where(hit, jnp.int32(kk), k)
                weight = jnp.where(hit, jnp.float32(1.0), weight)
            picks.append((k, weight))
        return picks

    for load in lists:
        load.wait()
    merged = 1
    picked = [pick(targets[i]) for i in range(early)]
    parts = []
    for m in range(members):
        for load in loads[m]:
            load.wait()
        blocks = [k_ref[m, :, 0 : CS * 128]] + [chosen(m, picked[i][m][0]) for i in range(merged)]
        made = jnp.dot(
            w_ref[m], jnp.concatenate(blocks, axis=1), preferred_element_type=jnp.float32
        ).astype(jnp.bfloat16)
        y_ref[m, :, 0 : CS * 128] = made[:, 0 : CS * 128]
        parts.append(
            lax.dot_general(
                made[:, CS * 128 :],
                made[:, 0 : CS * 128],
                (((0,), (0,)), ((), ())),
                preferred_element_type=jnp.float32,
            )
        )
    for i in range(early):
        if i >= merged:
            made = []
            for m in range(members):
                block = jnp.dot(
                    w_ref[m], chosen(m, picked[i][m][0]), preferred_element_type=jnp.float32
                ).astype(jnp.bfloat16)
                made.append(
                    lax.dot_general(
                        block,
                        y_ref[m, :, 0 : CS * 128],
                        (((0,), (0,)), ((), ())),
                        preferred_element_type=jnp.float32,
                    )
                )
        else:
            made = [part[i * 128 : (i + 1) * 128] for part in parts]
        total = made[0] * picked[i][0][1]
        for m in range(1, members):
            total = total + made[m] * picked[i][m][1]
        for j in range(CS):
            send_ref[(j * rows + i) * 128 : (j * rows + i + 1) * 128] = total[
                :, j * 128 : (j + 1) * 128
            ]
        if i == 0:
            met = 3 * len(sides) - 1
            pl.semaphore_wait(barrier, jnp.where(inner, met + len(sides) + fourth - 1, met))

            @pl.when(inner)
            def _():
                for n in range(1, fourth):
                    pl.semaphore_signal(
                        ready_sem, inc=1, device_id=(within(plane, n), col_at), device_id_type=MESH
                    )

        launch(i)
        if i == 0:
            given = pltpu.make_async_copy(boundary_ref, given_ref, given_sem)
            given.start()

    pl.semaphore_wait(ready_sem, jnp.where(inner, fourth - 1, 1))

    @pl.when(inner)
    def _():
        pl.semaphore_signal(
            ready_sem, inc=1, device_id=(within(mate, 0), col_at), device_id_type=MESH
        )

    for m in range(members):
        for n in range(CS * 128, slots * 128, 256):
            y_ref[m, :, n : n + 256] = jnp.dot(
                w_ref[m], columns(m, n // 128), preferred_element_type=jnp.float32
            ).astype(jnp.bfloat16)
        for n in range(0, slots, 2):
            part = lax.dot_general(
                y_ref[m, :, n * 128 : n * 128 + 256],
                y_ref[m, :, 0 : CS * 128],
                (((0,), (0,)), ((), ())),
                preferred_element_type=jnp.float32,
            )
            for d in range(2):
                for j in range(CS):
                    p_ref[m * slots + n + d, j] = part[
                        d * 128 : (d + 1) * 128, j * 128 : (j + 1) * 128
                    ]

    for i in range(early, rows):
        picks = pick(targets[i])
        for j in range(CS):
            total = p_ref[picks[0][0], j] * picks[0][1]
            for m in range(1, members):
                total = total + p_ref[m * slots + picks[m][0], j] * picks[m][1]
            ref, at = staged(i, j)
            ref[at : at + 128] = total
        if early < i <= late:
            launch(i - 1)
    launch(rows - 1)

    @pl.when(jnp.logical_not(inner))
    def _():
        for i in range(late, rows - 1):
            launch(i)

    def add_source(r, carry):
        for j in range(CS):
            first = (r * cols + lax.rem(col_at + cols - j, cols)) * members
            cell = jnp.int32(0)
            column = lax.div(ids_ref[j, first], cols)
            for m in range(members):
                for kk in range(slots):
                    if m > 0 and kk < CS:
                        continue
                    ident = ids_ref[kk, first + m]
                    cell = jnp.where(
                        lax.rem(ident, rows) == row_at,
                        lax.div(ident, rows) * cq + column,
                        cell,
                    )
            cell_ref[j * rows + r] = cell
        return carry

    lax.fori_loop(0, rows, add_source, 0)
    for i in range(fourth):
        for j in range(CS):
            cell_ref[sources + i * CS + j] = cell_ref[j * rows + within(far_mid, i)]
    listed = pltpu.make_async_copy(cell_ref, cells_ref, cell_sem)
    listed.start()

    given.wait()
    tall = given_ref.shape[1]

    def widen(q, carry):
        head_ref[q] = given_ref[q, :split].astype(jnp.float32).reshape(split * cq, 128)
        rest_ref[q] = given_ref[q, split:].astype(jnp.float32).reshape((tall - split) * cq, 128)
        return carry

    lax.fori_loop(0, nq, widen, 0)
    listed.wait()

    def settled(tiles):
        arrived = recv_ref.at[pl.ds(0, tiles * 128)]
        pltpu.make_async_copy(arrived, arrived, recv_sem).wait()
        sent = send_ref.at[pl.ds(0, (tiles - 1) * 128)]
        pltpu.make_async_copy(sent, sent, send_sem).wait()

    @pl.when(inner)
    def _():
        settled(sources - fourth * CS)

    @pl.when(jnp.logical_not(inner))
    def _():
        settled(sources)


def write_kernel(
    sources, cq, split,
    head_in_ref, rest_in_ref, recv_ref, cells_ref,
    out_ref, head_ref, rest_ref,
    cell_ref, cell_sem, sem,
):
    listed = pltpu.make_async_copy(cells_ref, cell_ref, cell_sem)
    listed.start()
    listed.wait()
    nq = head_ref.shape[0]
    tall = out_ref.shape[1] // cq

    for ref, start, height in ((head_ref, 0, split), (rest_ref, split, tall - split)):

        def settle(s, carry):
            cell = cell_ref[s]
            at = (lax.div(cell, cq), pl.ds(lax.rem(cell, cq), height, stride=cq), slice(None))
            ref[at] = ref[at] - recv_ref[pl.ds(pl.multiple_of(s * 128, 128) + start, height)]
            return carry

        lax.fori_loop(0, sources, settle, 0)
        for q in range(nq):
            pltpu.make_async_copy(
                ref.at[q], out_ref.at[q, pl.ds(start * cq, height * cq)], sem
            ).start()
    pltpu.make_async_copy(out_ref, out_ref, sem).wait()


def late_kernel(rows, cols, late_ref, after_ref, recv_ref, send_sem, recv_sem):
    row_at = lax.axis_index("row")
    col_at = lax.axis_index("col")
    sides = (0, 1) if cols == 2 else (0, 1, cols - 1)
    barrier = pltpu.get_barrier_semaphore()
    partners = [around(rows, row_at, 2 - row_at // (rows // 2), i) for i in range((rows // 4))]

    @pl.when(is_inner(rows, row_at))
    def _():
        for partner in partners:
            for j in sides:
                pl.semaphore_signal(
                    barrier, inc=1, device_id=(partner, lax.rem(col_at + j, cols)),
                    device_id_type=MESH,
                )
        pl.semaphore_wait(barrier, (rows // 4) * len(sides))
        for i, partner in enumerate(partners):
            for j in range(CS):
                part = pl.ds((i * CS + j) * 128, 128)
                pltpu.make_async_remote_copy(
                    src_ref=late_ref.at[part],
                    dst_ref=recv_ref.at[part],
                    send_sem=send_sem,
                    recv_sem=recv_sem,
                    device_id=(partner, lax.rem(col_at + j, cols)),
                    device_id_type=MESH,
                ).start()
        pltpu.make_async_copy(recv_ref, recv_ref, recv_sem).wait()
        pltpu.make_async_copy(late_ref, late_ref, send_sem).wait()


def patch_kernel(
    rows, sources, cq, split,
    result_ref, head_in_ref, rest_in_ref, recv_ref, cells_ref,
    out_ref, head_ref, rest_ref,
    sem,
):
    tall = out_ref.shape[1] // cq
    parts = ((head_ref, 0, split), (rest_ref, split, tall - split))

    @pl.when(is_inner(rows, lax.axis_index("row")))
    def _():
        listed = cells_ref[...]
        lane = lax.broadcasted_iota(jnp.int32, listed.shape, 0)
        cells = [
            jnp.sum(jnp.where(lane == sources + n, listed, 0)) for n in range((rows // 4) * CS)
        ]
        for n, cell in enumerate(cells):
            for ref, start, height in parts:
                at = (lax.div(cell, cq), pl.ds(lax.rem(cell, cq), height, stride=cq), slice(None))
                ref[at] = ref[at] - recv_ref[n * 128 + start : n * 128 + start + height]
        copies = []
        for cell in cells:
            q = lax.div(cell, cq)
            for ref, start, height in parts:
                copies.append(
                    pltpu.make_async_copy(
                        ref.at[q], out_ref.at[q, pl.ds(start * cq, height * cq)], sem
                    )
                )
                copies[-1].start()
        for copy in copies:
            copy.wait()


def kept(value):
    return pltpu.with_memory_space_constraint(value, pltpu.HBM)


def on_device(rows, cols, block_ids, iface_counts, inv_factor, coupling, boundary_block):
    slots = block_ids.shape[1]
    width = inv_factor.shape[1]
    members = inv_factor.shape[0] // width
    nq, tall, cq, _ = boundary_block.shape
    sources = CS * rows
    split = 48
    vmem = pl.BlockSpec(memory_space=pltpu.VMEM)
    hbm = pl.BlockSpec(memory_space=pltpu.HBM)
    head_shape = jax.ShapeDtypeStruct((nq, split * cq, 128), jnp.float32)
    rest_shape = jax.ShapeDtypeStruct((nq, (tall - split) * cq, 128), jnp.float32)
    late_shape = jax.ShapeDtypeStruct(((rows // 4) * CS * 128, 128), jnp.float32)
    result_shape = jax.ShapeDtypeStruct((nq, tall * cq, 128), jnp.float32)
    head, rest, landed, late, cells = pl.pallas_call(
        functools.partial(exchange_kernel, rows, cols, members, slots, width, nq, cq, split),
        out_shape=(
            head_shape,
            rest_shape,
            jax.ShapeDtypeStruct((sources * 128, 128), jnp.float32),
            late_shape,
            jax.ShapeDtypeStruct((sources + (rows // 4) * CS,), jnp.int32),
        ),
        in_specs=[hbm] * 5,
        out_specs=(vmem, vmem, vmem, vmem, hbm),
        scratch_shapes=[
            pltpu.SMEM((slots, block_ids.shape[0]), jnp.int32),
            pltpu.SMEM((block_ids.shape[0],), jnp.int32),
            pltpu.VMEM((members, width, width), jnp.bfloat16),
            pltpu.VMEM((members, width, slots * 128), jnp.bfloat16),
            pltpu.VMEM((members, width, slots * 128), jnp.bfloat16),
            pltpu.VMEM((members * slots, CS, 128, 128), jnp.float32),
            pltpu.VMEM((sources * 128, 128), jnp.float32),
            pltpu.VMEM(boundary_block.shape, jnp.bfloat16),
            pltpu.SMEM((sources + (rows // 4) * CS,), jnp.int32),
            pltpu.SemaphoreType.DMA((2,)),
            pltpu.SemaphoreType.DMA((members, 2)),
            pltpu.SemaphoreType.DMA,
            pltpu.SemaphoreType.DMA,
            pltpu.SemaphoreType.DMA,
            pltpu.SemaphoreType.DMA,
            pltpu.SemaphoreType.REGULAR,
        ],
        compiler_params=pltpu.CompilerParams(
            collective_id=0, has_side_effects=True, vmem_limit_bytes=32 * 1024 * 1024
        ),
        name="exchange",
    )(
        kept(block_ids.T),
        kept(iface_counts),
        kept(inv_factor.reshape(members, width, width)),
        kept(coupling.reshape(members, width, slots * 128)),
        kept(boundary_block),
    )
    local = [
        pltpu.SMEM((sources + (rows // 4) * CS,), jnp.int32),
        pltpu.SemaphoreType.DMA,
        pltpu.SemaphoreType.DMA,
    ]
    result, head, rest = pl.pallas_call(
        functools.partial(write_kernel, sources, cq, split),
        out_shape=(result_shape, head_shape, rest_shape),
        in_specs=[vmem, vmem, vmem, hbm],
        out_specs=(hbm, vmem, vmem),
        input_output_aliases={0: 1, 1: 2},
        scratch_shapes=local,
        compiler_params=pltpu.CompilerParams(vmem_limit_bytes=16 * 1024 * 1024),
        name="writing",
    )(head, rest, landed, cells)
    landed = pl.pallas_call(
        functools.partial(late_kernel, rows, cols),
        out_shape=late_shape,
        in_specs=[vmem, vmem],
        out_specs=vmem,
        scratch_shapes=[pltpu.SemaphoreType.DMA, pltpu.SemaphoreType.DMA],
        compiler_params=pltpu.CompilerParams(
            collective_id=1, has_side_effects=True, vmem_limit_bytes=16 * 1024 * 1024
        ),
        name="late",
    )(late, rest)
    result, _, _ = pl.pallas_call(
        functools.partial(patch_kernel, rows, sources, cq, split),
        out_shape=(result_shape, head_shape, rest_shape),
        in_specs=[hbm, vmem, vmem, vmem, vmem],
        out_specs=(hbm, vmem, vmem),
        input_output_aliases={0: 0, 1: 1, 2: 2},
        scratch_shapes=local[2:],
        compiler_params=pltpu.CompilerParams(vmem_limit_bytes=16 * 1024 * 1024),
        name="patching",
    )(result, head, rest, landed, cells)
    return result.reshape(boundary_block.shape)


def solution(mesh):
    return jax.shard_map(
        functools.partial(on_device, mesh.shape["row"], mesh.shape["col"]),
        mesh=mesh,
        in_specs=(
            P(),
            P(),
            P(("row", "col"), None),
            P(("row", "col"), None),
            P(None, "row", None, "col"),
        ),
        out_specs=P(None, "row", None, "col"),
        check_vma=False,
    )
```
